32 devices in a mesh: row: 4 (over x, core), col: 8 (over z, y).
Axes of the slice: x: 2, y: 2, z: 4, core: 2. Of those that a mesh axis runs over, the one named last changes fastest.
Arguments:
- basis_raw: float32 [37, 192, 1024], P(None, 'row', 'col'), may hold values from -4 to 4
- krylov_raw: float32 [4, 37, 34], replicated, may hold values from -6 to 6
- stiffness: float32 [192, 1024], P('row', 'col'), may hold values from -0.4 to 0.4
- rotation: float32 [192, 1024], P('row', 'col'), may hold values from -0.2 to 0.2
Outputs:
- new_columns: float32 [3, 192, 1024], P(None, 'row', 'col')
- coefficients: float32 [4, 40, 37], replicated
- hessenberg: float32 [3, 37], replicated
- gram: float32 [5, 40, 5, 40], replicated
- new_images: float32 [3, 192, 1024], P(None, 'row', 'col')
The draws below stay inside these ranges and needn't reach their ends.
All inputs are finite; a program needn't handle non-finite values.
Results may differ from the reference program's by a relative error of at most 0.001.
Values sent between devices are 32-bit elements; how exact they have to be, the bound alone decides.
No kernel may reach another device: no remote copies, remote signals or barrier semaphores. Data moves between devices by JAX's collectives and lax.ppermute only.
A program may use at most 64 MiB of HBM per device.

```python
import math
import jax
import jax.numpy as jnp
from jax import lax

K = 40
STEPS = 3
R = 37
KRYLOV = 34
NX = 192
NY = 1024


def draw_basis_raw(key, part):
    subkeys = jax.random.split(jax.random.fold_in(key, 17), 7)
    mode_count = R
    row_rate = jax.random.uniform(subkeys[0], (mode_count,), jnp.float32, 0.05, 3.0)
    col_rate = jax.random.uniform(subkeys[1], (mode_count,), jnp.float32, 0.05, 3.0)
    row_phase = jax.random.uniform(subkeys[2], (mode_count,), jnp.float32, 0.0, 2.0 * math.pi)
    col_phase = jax.random.uniform(subkeys[3], (mode_count,), jnp.float32, 0.0, 2.0 * math.pi)
    row_place = jnp.arange(NX, dtype=jnp.float32)
    col_place = jnp.arange(NY, dtype=jnp.float32)
    row_wave = jnp.cos(row_rate[:, None] * row_place[None, :] + row_phase[:, None])
    col_wave = jnp.cos(col_rate[:, None] * col_place[None, :] + col_phase[:, None])
    mixing = jax.random.uniform(subkeys[4], (R, mode_count), jnp.float32, -1.0, 1.0) * (2.0 / math.sqrt(mode_count))
    jitter = jax.random.uniform(subkeys[6], (R, NX, NY), jnp.float32, -0.3, 0.3)
    scaled_rows = mixing[:, :, None] * row_wave[None, :, :]
    smooth = jnp.einsum('rmx,my->rxy', scaled_rows, col_wave, precision=lax.Precision.HIGHEST)
    return jnp.clip(smooth + jitter, -4.0, 4.0)


def block_levels(rng, dims, cuts, smallest, high):
    factor_of, own = 1.0, jax.random.fold_in(rng, 6)
    for dim, shards_of in cuts:
        heights = jnp.exp(jax.random.uniform(jax.random.fold_in(own, dim), (shards_of,), jnp.float32, smallest / len(cuts), high / len(cuts)))
        factor_of = factor_of * jnp.repeat(heights, dims[dim] // shards_of).reshape([-1 if axis == dim else 1 for axis in range(len(dims))])
    return factor_of


def centred(own_key, extent, deviation, bound, held_as=jnp.bfloat16):
    array = jax.random.normal(own_key, extent, jnp.float32) * deviation
    return jnp.minimum(jnp.maximum(array, -bound), bound).astype(held_as)


def setup_inputs(seed: int = 0) -> dict:
    splits = jax.random.split(jax.random.key(seed), 5)
    basis_raw = draw_basis_raw(jax.random.fold_in(splits[4], 71), 0)
    krylov_raw = centred(splits[1], (4, R, KRYLOV), 1.0, 6.0, jnp.float32)
    stiffness = jnp.clip(jax.random.uniform(splits[2], (NX, NY), jnp.float32, -0.4, 0.4) * block_levels(splits[2], (NX, NY), ((0, 4), (1, 8)), -0.4, 0.0), -0.4, 0.4)
    rotation = jnp.clip(jax.random.uniform(splits[3], (NX, NY), jnp.float32, -0.2, 0.2) * block_levels(splits[3], (NX, NY), ((0, 4), (1, 8)), -0.4, 0.0), -0.2, 0.2)
    return {"basis_raw": basis_raw, "krylov_raw": krylov_raw, "stiffness": stiffness, "rotation": rotation}


COUPLING = 0.2
EPSILON = 1e-06
GRAM_SHIFT = 0.05
HIGHEST = lax.Precision.HIGHEST

def apply_core(border, diagonal, spin_field):
    middle = border[..., 1:-1, 1:-1]
    left_cells = border[..., 1:-1, :-2]
    right_cells = border[..., 1:-1, 2:]
    upper_cells = border[..., :-2, 1:-1]
    lower_cells = border[..., 2:, 1:-1]
    return diagonal * middle - COUPLING * (upper_cells + lower_cells + left_cells + right_cells) + spin_field * (right_cells - left_cells)

def lower_inverse(matrix):
    factor = jnp.linalg.cholesky(matrix)
    identity = jnp.eye(matrix.shape[0], dtype=matrix.dtype)
    return lax.linalg.triangular_solve(factor, identity, left_side=True, lower=True)

def reference(basis_raw, krylov_raw, stiffness, rotation):
    grid_total = NX * NY
    inverse_total = 1.0 / grid_total
    flat_raw = basis_raw.reshape(R, grid_total)
    raw_gram = jnp.dot(flat_raw, flat_raw.T, precision=HIGHEST) * inverse_total
    shifted = raw_gram + GRAM_SHIFT * jnp.eye(R, dtype=raw_gram.dtype)
    prepared = jnp.dot(lower_inverse(shifted), flat_raw, precision=HIGHEST)
    basis_rows = jnp.concatenate([prepared, jnp.zeros((STEPS, grid_total), prepared.dtype)], 0)
    krylov_flat = krylov_raw.reshape(4 * R, KRYLOV)
    krylov_ortho = jnp.dot(krylov_flat, lower_inverse(jnp.dot(krylov_flat.T, krylov_flat, precision=HIGHEST)).T, precision=HIGHEST)
    krylov_width = KRYLOV + STEPS
    krylov_rows = jnp.pad(krylov_ortho.reshape(4, R, KRYLOV), ((0, 0), (0, STEPS), (0, STEPS)))

    def operate(source):
        padding = [(0, 0)] * (source.ndim - 2) + [(1, 1), (1, 1)]
        return apply_core(jnp.pad(source, padding), stiffness, rotation)
    hessen_rows = []
    for turn_index in range(STEPS):
        column = KRYLOV + turn_index
        new_row = R + turn_index
        latest = krylov_rows[:, :, column - 1]
        components = jnp.dot(latest, basis_rows, precision=HIGHEST).reshape(4, NX, NY)
        section_four = components[3]
        section_three = components[2] + 2.0 * operate(section_four)
        section_two = components[1] + 2.0 * operate(section_three) - section_four
        section_one = components[0] + 2.0 * operate(section_two) - section_three
        summed = operate(section_one) - section_two
        target = (0.5 * components[2] - 0.5 * summed).reshape(grid_total)
        first_coef = jnp.dot(basis_rows, target, precision=HIGHEST) * inverse_total
        residual_one = target - jnp.dot(first_coef, basis_rows, precision=HIGHEST)
        second_coef = jnp.dot(basis_rows, residual_one, precision=HIGHEST) * inverse_total
        residual_two = residual_one - jnp.dot(second_coef, basis_rows, precision=HIGHEST)
        new_norm = jnp.sqrt(jnp.sum(residual_two * residual_two) * inverse_total + EPSILON)
        basis_rows = basis_rows.at[new_row].set(residual_two / new_norm)
        unit_row = (jnp.arange(K) == new_row).astype(basis_rows.dtype)
        expanded = jnp.stack([latest[1], 0.5 * (latest[0] + latest[2]), 0.5 * (latest[1] + latest[3]), first_coef + second_coef + new_norm * unit_row]).reshape(4 * K)
        matrix_view = krylov_rows.reshape(4 * K, krylov_width)
        first_proj = jnp.dot(expanded, matrix_view, precision=HIGHEST)
        ortho_one = expanded - jnp.dot(matrix_view, first_proj, precision=HIGHEST)
        second_proj = jnp.dot(ortho_one, matrix_view, precision=HIGHEST)
        ortho_two = ortho_one - jnp.dot(matrix_view, second_proj, precision=HIGHEST)
        krylov_norm = jnp.sqrt(jnp.sum(ortho_two * ortho_two) + EPSILON)
        krylov_rows = krylov_rows.at[:, :, column].set((ortho_two / krylov_norm).reshape(4, K))
        unit_column = (jnp.arange(krylov_width) == column).astype(krylov_rows.dtype)
        hessen_rows.append(first_proj + second_proj + krylov_norm * unit_column)
    new_columns = basis_rows[R:].reshape(STEPS, NX, NY)
    image_one = operate(new_columns)
    image_two = 2.0 * operate(image_one) - new_columns
    image_three = 2.0 * operate(image_two) - image_one
    new_images = 2.0 * operate(image_three) - image_two
    padded_basis = jnp.pad(basis_rows.reshape(K, NX, NY), ((0, 0), (4, 4), (0, 0)))
    diag_padded = jnp.pad(stiffness, ((4, 4), (0, 0)))
    spin_padded = jnp.pad(rotation, ((4, 4), (0, 0)))
    band_height = 32

    def row_apply(source, band_start, margin):
        out_rows = band_height + 2 * (margin - 1)
        diagonal = lax.dynamic_slice_in_dim(diag_padded, band_start + 5 - margin, out_rows, 0)
        spin_field = lax.dynamic_slice_in_dim(spin_padded, band_start + 5 - margin, out_rows, 0)
        result = apply_core(jnp.pad(source, ((0, 0), (0, 0), (1, 1))), diagonal, spin_field)
        row_global = band_start - (margin - 1) + jnp.arange(out_rows, dtype=jnp.int32)
        valid_rows = ((row_global >= 0) & (row_global < NX)).astype(result.dtype)
        return result * valid_rows[:, None]

    def crop_rows(source, margin):
        return source[:, margin:source.shape[1] - margin]

    def band_gram(gram_sum, band_start):
        order_zero = lax.dynamic_slice_in_dim(padded_basis, band_start, band_height + 8, 1)
        order_one = row_apply(order_zero, band_start, 4)
        order_two = 2.0 * row_apply(order_one, band_start, 3) - crop_rows(order_zero, 2)
        order_three = 2.0 * row_apply(order_two, band_start, 2) - crop_rows(order_one, 2)
        order_four = 2.0 * row_apply(order_three, band_start, 1) - crop_rows(order_two, 2)
        band_tile = jnp.concatenate([crop_rows(order_zero, 4), crop_rows(order_one, 3), crop_rows(order_two, 2), crop_rows(order_three, 1), order_four], 0).reshape(5 * K, band_height * NY)
        return (gram_sum + jnp.dot(band_tile, band_tile.T, precision=HIGHEST), None)
    band_starts = jnp.arange(NX // band_height, dtype=jnp.int32) * band_height
    gram_sum, _ = lax.scan(band_gram, jnp.zeros((5 * K, 5 * K), padded_basis.dtype), band_starts)
    gram = (gram_sum * inverse_total).reshape(5, K, 5, K)
    return (new_columns, krylov_rows, jnp.stack(hessen_rows), gram, new_images)
```

```python
import jax
import jax.numpy as jnp
from jax import lax
from jax.sharding import PartitionSpec as P

K = 40
STEPS = 3
R = 37
KRYLOV = 34


COUPLING = 0.2
EPSILON = 1e-06
GRAM_SHIFT = 0.05
HIGHEST = lax.Precision.HIGHEST


def padded(x, sides, width):
    for axis, dim in sides:
        peers, length = (lax.axis_size(axis), x.shape[dim])
        up = [(i, (i + 1) % peers) for i in range(peers - 1)]
        down = [(j, i) for i, j in up]
        last = lax.slice_in_dim(x, length - width, length, axis=dim)
        initial = lax.slice_in_dim(x, 0, width, axis=dim)
        before = lax.ppermute(last, axis, up)
        after = lax.ppermute(initial, axis, down)
        x = jnp.concatenate([before, x, after], axis=dim)
    return x


def apply_core(border, diagonal, spin_field):
    middle = border[..., 1:-1, 1:-1]
    left_cells = border[..., 1:-1, :-2]
    right_cells = border[..., 1:-1, 2:]
    upper_cells = border[..., :-2, 1:-1]
    lower_cells = border[..., 2:, 1:-1]
    return (
        diagonal * middle
        - COUPLING * (upper_cells + lower_cells + left_cells + right_cells)
        + spin_field * (right_cells - left_cells)
    )


def small_total(x):
    count = lax.axis_size("row") * lax.axis_size("col")
    spread = jnp.broadcast_to(x.reshape(1, -1), (count, x.size))
    parts = lax.all_to_all(spread, ("row", "col"), 0, 0, tiled=True)
    return jnp.sum(parts, axis=0).reshape(x.shape)


def large_total(x):
    count = lax.axis_size("row") * lax.axis_size("col")
    piece = -(-x.size // count)
    flat = jnp.pad(x.reshape(-1), (0, piece * count - x.size)).reshape(count, piece)
    mine = jnp.sum(lax.all_to_all(flat, ("row", "col"), 0, 0, tiled=True), axis=0)
    spread = jnp.broadcast_to(mine[None], (count, piece))
    whole = lax.all_to_all(spread, ("row", "col"), 0, 0, tiled=True)
    return whole.reshape(-1)[: x.size].reshape(x.shape)


def lower_inverse(matrix):
    factor = jnp.linalg.cholesky(matrix)
    identity = jnp.eye(matrix.shape[0], dtype=matrix.dtype)
    return lax.linalg.triangular_solve(factor, identity, left_side=True, lower=True)


def trimmed(source, margin):
    if margin == 0:
        return source
    return source[..., margin:-margin, margin:-margin]


def inside_mask(margin, row_count, col_count):
    row_first = lax.axis_index("row") * row_count - margin
    col_first = lax.axis_index("col") * col_count - margin
    row_global = row_first + lax.iota(jnp.int32, row_count + 2 * margin)
    col_global = col_first + lax.iota(jnp.int32, col_count + 2 * margin)
    row_valid = (row_global >= 0) & (row_global < row_count * lax.axis_size("row"))
    col_valid = (col_global >= 0) & (col_global < col_count * lax.axis_size("col"))
    return (row_valid[:, None] & col_valid[None, :]).astype(jnp.float32)


def local(basis_raw, krylov_raw, stiffness, rotation):
    row_count = basis_raw.shape[1]
    col_count = basis_raw.shape[2]
    cell_count = row_count * col_count
    grid_total = cell_count * lax.axis_size("row") * lax.axis_size("col")
    inverse_total = 1.0 / grid_total
    flat_raw = basis_raw.reshape(R, cell_count)
    raw_gram = (
        small_total(jnp.dot(flat_raw, flat_raw.T, precision=HIGHEST)) * inverse_total
    )
    inverse_factor = lower_inverse(raw_gram + GRAM_SHIFT * jnp.eye(R, dtype=jnp.float32))
    prepared = jnp.dot(inverse_factor, flat_raw, precision=HIGHEST)
    basis_rows = jnp.concatenate([prepared, jnp.zeros((STEPS, cell_count), jnp.float32)], 0)
    krylov_flat = krylov_raw.reshape(4 * R, KRYLOV)
    krylov_ortho = jnp.dot(
        krylov_flat,
        lower_inverse(jnp.dot(krylov_flat.T, krylov_flat, precision=HIGHEST)).T,
        precision=HIGHEST,
    )
    krylov_width = KRYLOV + STEPS
    krylov_rows = jnp.pad(krylov_ortho.reshape(4, R, KRYLOV), ((0, 0), (0, STEPS), (0, STEPS)))
    field_rim = padded(jnp.stack([stiffness, rotation]), (("row", 1), ("col", 2)), 3)

    def shrink(extended, margin):
        diagonal = trimmed(field_rim[0], 4 - margin)
        spin_field = trimmed(field_rim[1], 4 - margin)
        return apply_core(extended, diagonal, spin_field) * inside_mask(
            margin - 1, row_count, col_count
        )

    hessen_rows = []
    for turn_index in range(STEPS):
        column = KRYLOV + turn_index
        new_row = R + turn_index
        latest = krylov_rows[:, :, column - 1]
        components = jnp.dot(latest, basis_rows, precision=HIGHEST).reshape(4, row_count, col_count)
        block_rim = padded(components, (("row", 1), ("col", 2)), 4)
        section_four = block_rim[3]
        section_three = trimmed(block_rim[2], 1) + 2.0 * shrink(section_four, 4)
        section_two = (
            trimmed(block_rim[1], 2) + 2.0 * shrink(section_three, 3) - trimmed(section_four, 2)
        )
        section_one = (
            trimmed(block_rim[0], 3) + 2.0 * shrink(section_two, 2) - trimmed(section_three, 2)
        )
        summed = shrink(section_one, 1) - trimmed(section_two, 2)
        target = (0.5 * components[2] - 0.5 * summed).reshape(cell_count)
        first_coef = (
            small_total(jnp.dot(basis_rows, target, precision=HIGHEST)) * inverse_total
        )
        residual_one = target - jnp.dot(first_coef, basis_rows, precision=HIGHEST)
        second_coef = (
            small_total(jnp.dot(basis_rows, residual_one, precision=HIGHEST))
            * inverse_total
        )
        residual_two = residual_one - jnp.dot(second_coef, basis_rows, precision=HIGHEST)
        square = small_total(jnp.sum(residual_two * residual_two)) * inverse_total
        new_norm = jnp.sqrt(square + EPSILON)
        basis_rows = basis_rows.at[new_row].set(residual_two / new_norm)
        unit_row = (jnp.arange(K) == new_row).astype(jnp.float32)
        expanded = jnp.stack(
            [
                latest[1],
                0.5 * (latest[0] + latest[2]),
                0.5 * (latest[1] + latest[3]),
                first_coef + second_coef + new_norm * unit_row,
            ]
        ).reshape(4 * K)
        matrix_view = krylov_rows.reshape(4 * K, krylov_width)
        first_proj = jnp.dot(expanded, matrix_view, precision=HIGHEST)
        ortho_one = expanded - jnp.dot(matrix_view, first_proj, precision=HIGHEST)
        second_proj = jnp.dot(ortho_one, matrix_view, precision=HIGHEST)
        ortho_two = ortho_one - jnp.dot(matrix_view, second_proj, precision=HIGHEST)
        krylov_norm = jnp.sqrt(jnp.sum(ortho_two * ortho_two) + EPSILON)
        krylov_rows = krylov_rows.at[:, :, column].set((ortho_two / krylov_norm).reshape(4, K))
        unit_column = (jnp.arange(krylov_width) == column).astype(jnp.float32)
        hessen_rows.append(first_proj + second_proj + krylov_norm * unit_column)
    new_columns = basis_rows[R:].reshape(STEPS, row_count, col_count)
    order_zero = padded(basis_rows.reshape(K, row_count, col_count), (("row", 1), ("col", 2)), 4)
    order_one = shrink(order_zero, 4)
    order_two = 2.0 * shrink(order_one, 3) - trimmed(order_zero, 2)
    order_three = 2.0 * shrink(order_two, 2) - trimmed(order_one, 2)
    order_four = 2.0 * shrink(order_three, 1) - trimmed(order_two, 2)
    polynomials = [
        trimmed(order_zero, 4),
        trimmed(order_one, 3),
        trimmed(order_two, 2),
        trimmed(order_three, 1),
        order_four,
    ]
    new_images = polynomials[4][R:]
    band_rows = row_count // 8

    def accumulate(band_index, gram_sum):
        band_start = band_index * band_rows
        band_tile = jnp.concatenate(
            [
                lax.dynamic_slice_in_dim(poly_field, band_start, band_rows, 1).reshape(
                    K, band_rows * col_count
                )
                for poly_field in polynomials
            ],
            0,
        )
        return gram_sum + jnp.dot(band_tile, band_tile.T, precision=HIGHEST)

    local_gram = lax.fori_loop(0, 8, accumulate, jnp.zeros((5 * K, 5 * K), jnp.float32))
    gram = (large_total(local_gram) * inverse_total).reshape(5, K, 5, K)
    return (new_columns, krylov_rows, jnp.stack(hessen_rows), gram, new_images)


def solution(mesh):
    in_specs = (P(None, "row", "col"), P(), P("row", "col"), P("row", "col"))
    out_specs = (P(None, "row", "col"), P(), P(), P(), P(None, "row", "col"))
    return jax.shard_map(local, mesh=mesh, in_specs=in_specs, out_specs=out_specs, check_vma=False)
```

```python
import functools
import jax
import jax.numpy as jnp
from jax import lax
from jax.experimental import pallas as pl
from jax.experimental.pallas import tpu as pltpu
from jax.sharding import PartitionSpec as P

K = 40
STEPS = 3
R = 37
KRYLOV = 34
WIDTH = KRYLOV + STEPS

COUPLING = 0.2
EPSILON = 1e-06
GRAM_SHIFT = 0.05
HIGHEST = lax.Precision.HIGHEST
F32 = jnp.float32
BF16 = jnp.bfloat16

ORDERS = 5
HALO = (ORDERS - 1) * (STEPS + 1)
STRIDE = 48
WIDE = 256
PAD = 128
AXES = ("row", "col")
NT = (((1,), (1,)), ((), ()))


def lower_inverse(matrix):
    factor = jnp.linalg.cholesky(matrix)
    identity = jnp.eye(matrix.shape[0], dtype=matrix.dtype)
    return lax.linalg.triangular_solve(factor, identity, left_side=True, lower=True)


def device_count():
    return lax.axis_size("row") * lax.axis_size("col")


def exchange(spread):
    return lax.all_to_all(spread, AXES, 0, 0, tiled=True)


def shifts(axis):
    peers = lax.axis_size(axis)
    up = [(i, i + 1) for i in range(peers - 1)]
    return up, [(j, i) for i, j in up]


def lanes(shape):
    return lax.broadcasted_iota(jnp.int32, shape, len(shape) - 1)


def sublanes(shape):
    return lax.broadcasted_iota(jnp.int32, shape, len(shape) - 2)


def pack_body(tall_ref, low_ref, high_ref):
    total, slots, cols = tall_ref.shape
    span = cols // HALO
    lane = lanes((slots, cols))

    def group(g, carry):
        low = jnp.zeros((slots, cols), F32)
        high = jnp.zeros((slots, cols), F32)
        for k in range(span):
            cells = tall_ref[g * span + k]
            inside = (lane >= k * HALO) & (lane < (k + 1) * HALO)
            first = pltpu.roll(cells, k * HALO, 1) if k else cells
            turn = (k * HALO + HALO) % cols
            second = pltpu.roll(cells, turn, 1) if turn else cells
            low = jnp.where(inside, first, low)
            high = jnp.where(inside, second, high)
        low_ref[g] = low
        high_ref[g] = high
        return carry

    lax.fori_loop(0, total // span, group, 0)


def sideways(main, side, lane):
    cols = main.shape[-1]
    main_up = pltpu.roll(main, 1, 1)
    side_up = pltpu.roll(side, 1, 1)
    main_down = pltpu.roll(main, cols - 1, 1)
    side_down = pltpu.roll(side, cols - 1, 1)
    first = lane == 0
    last = lane == cols - 1
    left = (jnp.where(first, side_up, main_up), jnp.where(first, main_up, side_up))
    right = (jnp.where(last, side_down, main_down), jnp.where(last, main_down, side_down))
    return left, right


def image_body(
    tall_ref, left_ref, right_ref,
    main_ref, side_ref, coef_ref, hi_ref, lo_ref, gram_ref,
    local_ref, m1, s1, m2, s2, m3, s3, acc_ref,
):
    total, slots, cols = tall_ref.shape
    rows = total - 2 * HALO
    span = cols // HALO
    lane = lanes((slots, cols))
    field = sublanes((slots, cols))

    def unpack(g, carry):
        gathered = [[] for _ in range(8)]
        from_left = left_ref[g]
        from_right = right_ref[g]
        for k in range(span):
            r = g * span + k
            main = tall_ref[r]
            turn = (cols - k * HALO) % cols
            low = pltpu.roll(from_right, turn, 1) if turn else from_right
            turn = (cols - HALO - k * HALO) % cols
            high = pltpu.roll(from_left, turn, 1) if turn else from_left
            side = jnp.where(lane < HALO, low, jnp.where(lane >= cols - HALO, high, 0.0))
            packed = []
            for cells in (main, side):
                spin = cells[R + 1 : R + 2]
                couple = COUPLING * cells[R + 2 : R + 3]
                packed += [cells[R : R + 1], spin - couple, -spin - couple, couple]
            local_ref[r] = jnp.concatenate(packed, 0)
            for q in range(8):
                gathered[q].append(packed[q])
            main_ref[r] = jnp.where(field < R, main, 0.0)
            side_ref[r] = jnp.where(field < R, side, 0.0)
        for q in range(8):
            coef_ref[q, pl.ds(g * span, span), :] = jnp.concatenate(gathered[q], 0)
        return carry

    lax.fori_loop(0, total // span, unpack, 0)

    blank = jnp.zeros((STRIDE - slots, cols), F32)

    def keep(order, r, cells):
        whole = jnp.concatenate([cells, blank], 0)
        high = whole.astype(BF16)
        low = (whole - high.astype(F32)).astype(BF16)
        place = pl.ds(pl.multiple_of((r - HALO) * cols, cols), cols)
        hi_ref[order * STRIDE : (order + 1) * STRIDE, place] = high
        lo_ref[order * STRIDE : (order + 1) * STRIDE, place] = low

    def level(order, source, older, target, need_side):
        source_main, source_side = source

        def one(r, store):
            main = source_main[r]
            side = source_side[r]
            local = local_ref[r]
            left, right = sideways(main, side, lane)
            scale = 1.0 if order == 1 else 2.0
            fresh = scale * (
                local[0:1] * main
                + local[1:2] * right[0]
                + local[2:3] * left[0]
                - local[3:4] * (source_main[r - 1] + source_main[r + 1])
            )
            if older is not None:
                fresh = fresh - older[0][r]
            if target is not None:
                target[0][r] = fresh
            if need_side:
                edge = scale * (
                    local[4:5] * side
                    + local[5:6] * right[1]
                    + local[6:7] * left[1]
                    - local[7:8] * (source_side[r - 1] + source_side[r + 1])
                )
                if older is not None:
                    edge = edge - older[1][r]
                target[1][r] = edge
            if store:
                keep(order, r, fresh)

        reach = ORDERS - 1 - order

        def inner(r, carry):
            one(r, True)
            return carry

        def outer(r, carry):
            one(r, False)
            return carry

        if reach:
            lax.fori_loop(HALO - reach, HALO, outer, 0)
            lax.fori_loop(HALO + rows, HALO + rows + reach, outer, 0)
        lax.fori_loop(HALO, HALO + rows, inner, 0)

    def plain(r, carry):
        keep(0, r, main_ref[r])
        return carry

    lax.fori_loop(HALO, HALO + rows, plain, 0)
    level(1, (main_ref, side_ref), None, (m1, s1), True)
    level(2, (m1, s1), (main_ref, side_ref), (m2, s2), True)
    level(3, (m2, s2), (m1, s1), (m3, s3), True)
    level(4, (m3, s3), (m2, s2), None, False)

    size = ORDERS * STRIDE
    chunk = 4 * cols
    acc_ref[...] = jnp.zeros(acc_ref.shape, F32)

    def product(i, carry):
        place = pl.ds(pl.multiple_of(i * chunk, chunk), chunk)
        high = hi_ref[:, place]
        low = lo_ref[:, place]
        acc_ref[:, :size] += (
            lax.dot_general(high, high, NT, preferred_element_type=F32)
            + lax.dot_general(high, low, NT, preferred_element_type=F32)
            + lax.dot_general(low, high, NT, preferred_element_type=F32)
        )
        return carry

    lax.fori_loop(0, rows * cols // chunk, product, 0)
    lane_wide = lanes((K, WIDE))

    def band(order):
        return acc_ref[order * STRIDE : order * STRIDE + K, :]

    gram_ref[0:K] = band(0)
    gram_ref[K : 2 * K] = jnp.where(
        lane_wide < STRIDE, pltpu.roll(band(4), WIDE - 4 * STRIDE, 1), band(1)
    )
    gram_ref[2 * K : 3 * K] = jnp.where(
        lane_wide < 2 * STRIDE, pltpu.roll(band(3), WIDE - 3 * STRIDE, 1), band(2)
    )
    gram_ref[3 * K :] = jnp.zeros((gram_ref.shape[0] - 3 * K, WIDE), F32)


def absorb(parts, state, turn, inverse_total):
    gram, factor, flipped, square, vectors, pending = state
    new_row = R + turn
    column = KRYLOV + turn
    total = jnp.sum(parts, axis=0, keepdims=True) * inverse_total
    table = jnp.concatenate(
        [total[:, a * WIDE : (a + 1) * WIDE] for a in range(ORDERS)]
        + [jnp.zeros((8 - ORDERS, WIDE), F32)],
        0,
    )
    lane_one = lanes((1, WIDE))
    norm = jnp.sum(jnp.where(lane_one == new_row, table[0:1], 0.0), axis=1, keepdims=True)
    beta = jnp.sqrt(norm + EPSILON)
    sigma = 1.0 / beta
    here = (lanes((K, PAD)) == new_row) & (sublanes((K, PAD)) == new_row)
    factor = jnp.where(here, sigma, factor)
    flipped = jnp.where(here, sigma, flipped)
    square = jnp.where(here, sigma * sigma, square)
    tall = jnp.transpose(
        jnp.concatenate([table[:, :PAD], jnp.zeros((PAD - 8, PAD), F32)], 0)
    )
    lane_gram = lanes((K, WIDE))
    gram = jnp.where(sublanes((K, WIDE)) == new_row, table[0:1], gram)
    for b in range(ORDERS):
        gram = jnp.where(lane_gram == b * STRIDE + new_row, tall[:K, b : b + 1], gram)

    latest = [vectors[j * K : (j + 1) * K, column - 1 : column] for j in range(4)]
    unit = (lax.broadcasted_iota(jnp.int32, (K, 1), 0) == new_row).astype(F32)
    expanded = jnp.concatenate(
        [
            latest[1],
            0.5 * (latest[0] + latest[2]),
            0.5 * (latest[1] + latest[3]),
            pending + beta * unit,
        ],
        0,
    )
    first = jnp.sum(vectors * expanded, axis=0, keepdims=True)
    ortho = expanded - jnp.sum(vectors * first, axis=1, keepdims=True)
    second = jnp.sum(vectors * ortho, axis=0, keepdims=True)
    ortho = ortho - jnp.sum(vectors * second, axis=1, keepdims=True)
    eta = jnp.sqrt(jnp.sum(ortho * ortho, axis=0, keepdims=True) + EPSILON)
    vectors = jnp.where(lanes((4 * K, PAD)) == column, ortho / eta, vectors)
    hessenberg = first + second + eta * (lanes((1, PAD)) == column).astype(F32)
    return (gram, factor, flipped, square, vectors, pending), table, sigma, hessenberg


def coefficients_of(state, turn):
    gram, factor, flipped, square, vectors, _ = state
    column = KRYLOV + turn
    latest = [vectors[j * K : (j + 1) * K, column - 1 : column] for j in range(4)]
    mixes = [jnp.sum(factor * one, axis=0, keepdims=True) for one in latest]
    wide = [jnp.concatenate([m, jnp.zeros((1, WIDE - PAD), F32)], 1) for m in mixes]
    target = 0.5 * wide[2]
    for j in range(4):
        target = target - pltpu.roll(0.5 * wide[j], (j + 1) * STRIDE, 1)
    raw = jnp.sum(gram * target, axis=1, keepdims=True)
    upper = jnp.sum(square * raw, axis=0, keepdims=True)
    inside = jnp.where(lanes((K, PAD)) < K, gram[:, :PAD], 0.0)
    twice = 2.0 * raw - jnp.sum(inside * upper, axis=1, keepdims=True)
    removed = jnp.sum(square * twice, axis=0, keepdims=True)
    pending = jnp.sum(
        jnp.where(lanes((K, PAD)) == sublanes((K, PAD)), jnp.sum(flipped * twice, axis=0, keepdims=True), 0.0),
        axis=1,
        keepdims=True,
    )
    table = jnp.concatenate(mixes + [removed] + [jnp.zeros((PAD - 5, PAD), F32)], 0)
    return jnp.transpose(table), mixes + [removed], pending


def turn_body(turn, inverse_total, count, *refs):
    refs = list(refs)
    parts_ref = refs.pop(0) if turn else None
    state_refs = [refs.pop(0) for _ in range(6)]
    main_ref, side_ref, coef_ref, hi_ref, lo_ref = [refs.pop(0) for _ in range(5)]
    old_fields = [refs.pop(0) for _ in range(turn)]
    old_rows = [refs.pop(0) for _ in range(turn)]
    spread_ref, field_ref, rows_ref, image_ref = [refs.pop(0) for _ in range(4)]
    out_state = [refs.pop(0) for _ in range(6)]
    if turn:
        table_ref, sigma_ref, hessenberg_ref = [refs.pop(0) for _ in range(3)]
    z_ref, t_ref = refs

    state = tuple(r[...] for r in state_refs[:5]) + (state_refs[5][:, 0:1],)
    if turn:
        state, table, sigma, hessenberg = absorb(parts_ref[...], state, turn - 1, inverse_total)
        table_ref[...] = table
        sigma_ref[...] = jnp.broadcast_to(sigma, sigma_ref.shape)
        hessenberg_ref[...] = jnp.broadcast_to(hessenberg, hessenberg_ref.shape)
    upright, mixes, pending = coefficients_of(state, turn)
    for ref, value in zip(out_state[:5], state[:5]):
        ref[...] = value
    out_state[5][...] = jnp.broadcast_to(pending, out_state[5].shape)

    total, slots, cols = main_ref.shape
    rows = total - 2 * HALO
    weights = [jnp.broadcast_to(upright[:K, j : j + 1], (K, cols)) for j in range(5)]

    def mix(g, carry):
        lists = [[[], []] for _ in range(5)]
        for k in range(8):
            for half, ref in enumerate((main_ref, side_ref)):
                cells = ref[g * 8 + k]
                for j in range(5):
                    lists[j][half].append(jnp.sum(weights[j] * cells, axis=0, keepdims=True))
        for j in range(5):
            for half in range(2):
                z_ref[j, half, pl.ds(pl.multiple_of(g * 8, 8), 8), :] = jnp.concatenate(lists[j][half], 0)
        return carry

    lax.fori_loop(0, total // 8, mix, 0)

    z = []
    for j in range(5):
        pair = [z_ref[j, 0], z_ref[j, 1]]
        for s in range(turn):
            scale = mixes[j][:, R + s : R + s + 1]
            pair = [pair[half] + scale * old_fields[s][half] for half in range(2)]
        z.append(pair)

    lane = lanes((total, cols))
    local = [coef_ref[q] for q in range(8)]

    def operate(pair):
        main, side = pair
        left, right = sideways(main, side, lane)
        out = []
        for half, cells in enumerate(pair):
            c = local[4 * half : 4 * half + 4]
            out.append(
                c[0] * cells
                + c[1] * right[half]
                + c[2] * left[half]
                - c[3] * (pltpu.roll(cells, 1, 0) + pltpu.roll(cells, total - 1, 0))
            )
        return out

    def combine(*terms):
        return [sum(w * p[half] for w, p in terms) for half in range(2)]

    four = z[3]
    three = combine((1.0, z[2]), (2.0, operate(four)))
    two = combine((1.0, z[1]), (2.0, operate(three)), (-1.0, four))
    one = combine((1.0, z[0]), (2.0, operate(two)), (-1.0, three))
    summed = combine((1.0, operate(one)), (-1.0, two))
    field = combine((0.5, z[2]), (-0.5, summed), (-1.0, z[4]))
    field_ref[0] = field[0]
    field_ref[1] = field[1]

    images = [field, operate(field)]
    for _ in range(ORDERS - 2):
        images.append(combine((2.0, operate(images[-1])), (-1.0, images[-2])))
    for a in range(ORDERS):
        t_ref[a] = images[a][0]
    image_ref[...] = t_ref[ORDERS - 1, HALO : HALO + rows, :]
    rows_ref[...] = jnp.zeros(rows_ref.shape, F32)
    for r in range(rows):
        for a in range(ORDERS):
            rows_ref[a : a + 1, r * cols : (r + 1) * cols] = t_ref[a, HALO + r : HALO + r + 1, :]

    size = ORDERS * STRIDE
    chunk = 8 * cols
    table = jnp.zeros((8, size), F32)
    own = jnp.zeros((8, 8 * (turn + 1)), F32)
    for i in range(rows * cols // chunk):
        place = slice(i * chunk, (i + 1) * chunk)
        mine = rows_ref[:, place]
        rounded = mine.astype(BF16).astype(F32)
        both = jnp.concatenate([rounded, mine - rounded], 0).astype(BF16)
        by_high = lax.dot_general(both, hi_ref[:, place], NT, preferred_element_type=F32)
        by_low = lax.dot_general(both, lo_ref[:, place], NT, preferred_element_type=F32)
        table = table + (by_high[0:8] + by_high[8:16] + by_low[0:8])
        others = jnp.concatenate([ref[:, place] for ref in old_rows] + [mine], 0)
        own = own + lax.dot_general(mine, others, NT, precision=HIGHEST, preferred_element_type=F32)
    table = jnp.concatenate([table, jnp.zeros((8, WIDE - size), F32)], 1)
    lane_table = lanes((8, WIDE))
    for s in range(turn + 1):
        for b in range(ORDERS):
            table = jnp.where(
                lane_table == b * STRIDE + R + s, own[:, 8 * s + b : 8 * s + b + 1], table
            )
    flat = jnp.concatenate([table[a : a + 1] for a in range(ORDERS)], 1)
    spread_ref[...] = jnp.broadcast_to(flat, (count, ORDERS * WIDE))


def final_body(inverse_total, *refs):
    refs = list(refs)
    parts_ref = refs.pop(0)
    state_refs = [refs.pop(0) for _ in range(6)]
    folded_ref = refs.pop(0)
    old_tables = [refs.pop(0) for _ in range(STEPS - 1)]
    old_sigmas = [refs.pop(0) for _ in range(STEPS - 1)]
    fields = [refs.pop(0) for _ in range(STEPS)]
    images = [refs.pop(0) for _ in range(STEPS)]
    columns_ref, coefficients_ref, hessenberg_ref, gram_ref, image_ref = refs

    state = tuple(r[...] for r in state_refs[:5]) + (state_refs[5][:, 0:1],)
    state, table, sigma, hessenberg = absorb(parts_ref[...], state, STEPS - 1, inverse_total)
    factor = state[1]
    coefficients_ref[...] = state[4]
    hessenberg_ref[...] = jnp.broadcast_to(hessenberg, hessenberg_ref.shape)
    sigmas = [ref[0:1, 0:1] for ref in old_sigmas] + [sigma]
    rows = columns_ref.shape[1]
    for s in range(STEPS):
        columns_ref[s] = sigmas[s] * fields[s][0, HALO : HALO + rows, :]
        image_ref[s] = sigmas[s] * images[s][...]

    lane_wide = lanes((K, WIDE))
    bands = [folded_ref[i * K : (i + 1) * K, :] for i in range(3)]
    upper = [
        bands[0],
        bands[1],
        bands[2],
        pltpu.roll(bands[2], 3 * STRIDE, 1),
        pltpu.roll(bands[1], 4 * STRIDE, 1),
    ]
    blank = jnp.zeros((STRIDE - K, WIDE), F32)
    stacked = []
    for a in range(ORDERS):
        stacked += [jnp.where((lane_wide >= a * STRIDE) & (lane_wide < ORDERS * STRIDE), upper[a], 0.0), blank]
    whole = jnp.concatenate(stacked + [jnp.zeros((WIDE - ORDERS * STRIDE, WIDE), F32)], 0)
    row_id = sublanes((WIDE, WIDE))
    lane_id = lanes((WIDE, WIDE))
    lower = row_id >= (lane_id // STRIDE + 1) * STRIDE
    whole = jnp.where(lower, jnp.transpose(whole), whole)
    for s, one in enumerate([ref[...] for ref in old_tables] + [table]):
        flipped = jnp.transpose(jnp.concatenate([one, jnp.zeros((PAD - 8, WIDE), F32)], 0))
        for a in range(ORDERS):
            whole = jnp.where(row_id == a * STRIDE + R + s, one[a : a + 1, :], whole)
        for a in range(ORDERS):
            whole = jnp.where(lane_id == a * STRIDE + R + s, flipped[:, a : a + 1], whole)
    padded = jnp.concatenate([factor, jnp.zeros((K, WIDE - PAD), F32)], 1)
    padded = jnp.concatenate([padded, blank], 0)
    blocks = [padded] + [pltpu.roll(padded, a * STRIDE, 1) for a in range(1, ORDERS)]
    diagonal = jnp.concatenate(blocks + [jnp.zeros((WIDE - ORDERS * STRIDE, WIDE), F32)], 0)
    half = jnp.dot(diagonal, whole, precision=HIGHEST, preferred_element_type=F32)
    gram_ref[...] = lax.dot_general(half, diagonal, NT, precision=HIGHEST, preferred_element_type=F32)


def shape(*dims, dtype=F32):
    return jax.ShapeDtypeStruct(dims, dtype)


def local(basis_raw, krylov_raw, stiffness, rotation):
    rows = basis_raw.shape[1]
    cols = basis_raw.shape[2]
    cells = rows * cols
    count = device_count()
    inverse_total = 1.0 / (cells * count)
    total = rows + 2 * HALO
    size = ORDERS * STRIDE

    fields = jnp.concatenate(
        [
            jnp.transpose(basis_raw, (1, 0, 2)),
            stiffness[:, None],
            rotation[:, None],
            jnp.ones((rows, 1, cols), F32),
        ],
        1,
    )
    up, down = shifts("row")
    before = lax.ppermute(fields[rows - HALO :], "row", up)
    after = lax.ppermute(fields[:HALO], "row", down)
    tall = jnp.concatenate([before, fields, after], 0)
    strip = shape(total * HALO // cols, K, cols)
    low, high = pl.pallas_call(pack_body, out_shape=(strip, strip), name="pack")(tall)
    up, down = shifts("col")
    from_left = lax.ppermute(high, "col", up)
    from_right = lax.ppermute(low, "col", down)

    level = pltpu.VMEM((total, K, cols), F32)
    main, side, coefs, hi, lo, folded = pl.pallas_call(
        image_body,
        out_shape=(
            shape(total, K, cols),
            shape(total, K, cols),
            shape(8, total, cols),
            shape(size, cells, dtype=BF16),
            shape(size, cells, dtype=BF16),
            shape(PAD, WIDE),
        ),
        scratch_shapes=[pltpu.VMEM((total, 8, cols), F32)]
        + [level] * 6
        + [pltpu.VMEM((size, WIDE), F32)],
        name="images",
    )(tall, from_left, from_right)

    piece = PAD * WIDE // count
    mine = jnp.sum(exchange(folded.reshape(count, piece)), axis=0) * inverse_total
    folded = exchange(jnp.broadcast_to(mine[None], (count, piece))).reshape(PAD, WIDE)

    inverse_factor = lower_inverse(folded[:R, :R] + GRAM_SHIFT * jnp.eye(R, dtype=F32))
    krylov_flat = krylov_raw.reshape(4 * R, KRYLOV)
    krylov_ortho = jnp.dot(
        krylov_flat,
        lower_inverse(jnp.dot(krylov_flat.T, krylov_flat, precision=HIGHEST)).T,
        precision=HIGHEST,
    )
    vectors = jnp.pad(
        krylov_ortho.reshape(4, R, KRYLOV), ((0, 0), (0, K - R), (0, PAD - KRYLOV))
    ).reshape(4 * K, PAD)
    wide = ((0, K - R), (0, PAD - R))
    state = (
        folded[:K],
        jnp.pad(inverse_factor, wide),
        jnp.pad(inverse_factor.T, wide),
        jnp.pad(jnp.dot(inverse_factor.T, inverse_factor, precision=HIGHEST), wide),
        vectors,
        jnp.zeros((K, PAD), F32),
    )
    state_shapes = (
        shape(K, WIDE),
        shape(K, PAD),
        shape(K, PAD),
        shape(K, PAD),
        shape(4 * K, PAD),
        shape(K, PAD),
    )
    parts = ()
    made_fields, made_rows, made_images, tables, sigmas, hessen = [], [], [], [], [], []
    for turn in range(STEPS):
        out_shape = (
            shape(count, ORDERS * WIDE),
            shape(2, total, cols),
            shape(8, cells),
            shape(rows, cols),
        ) + state_shapes
        if turn:
            out_shape += (shape(8, WIDE), shape(8, PAD), shape(8, PAD))
        outs = pl.pallas_call(
            functools.partial(turn_body, turn, inverse_total, count),
            out_shape=out_shape,
            scratch_shapes=[
                pltpu.VMEM((5, 2, total, cols), F32),
                pltpu.VMEM((ORDERS, total, cols), F32),
            ],
            name=f"turn{turn}",
        )(*parts, *state, main, side, coefs, hi, lo, *made_fields, *made_rows)
        made_fields.append(outs[1])
        made_rows.append(outs[2])
        made_images.append(outs[3])
        state = outs[4:10]
        if turn:
            tables.append(outs[10])
            sigmas.append(outs[11])
            hessen.append(outs[12][0, :WIDTH])
        parts = (exchange(outs[0]),)

    new_columns, vectors, last, gram, new_images = pl.pallas_call(
        functools.partial(final_body, inverse_total),
        out_shape=(
            shape(STEPS, rows, cols),
            shape(4 * K, PAD),
            shape(8, PAD),
            shape(WIDE, WIDE),
            shape(STEPS, rows, cols),
        ),
        name="final",
    )(*parts, *state, folded, *tables, *sigmas, *made_fields, *made_images)
    hessen.append(last[0, :WIDTH])
    gram = gram[:size, :size].reshape(ORDERS, STRIDE, ORDERS, STRIDE)[:, :K, :, :K]
    coefficients = vectors.reshape(4, K, PAD)[:, :, :WIDTH]
    return (new_columns, coefficients, jnp.stack(hessen), gram, new_images)


def solution(mesh):
    in_specs = (P(None, "row", "col"), P(), P("row", "col"), P("row", "col"))
    out_specs = (P(None, "row", "col"), P(), P(), P(), P(None, "row", "col"))
    return jax.shard_map(local, mesh=mesh, in_specs=in_specs, out_specs=out_specs, check_vma=False)
```

```python
import functools
import jax
import jax.numpy as jnp
from jax import lax
from jax.experimental import pallas as pl
from jax.experimental.pallas import tpu as pltpu
from jax.sharding import PartitionSpec as P

K = 40
STEPS = 3
R = 37
KRYLOV = 34
WIDTH = KRYLOV + STEPS

COUPLING = 0.2
EPSILON = 1e-06
GRAM_SHIFT = 0.05
HIGHEST = lax.Precision.HIGHEST
F32 = jnp.float32
BF16 = jnp.bfloat16

ORDERS = 5
HALO = (ORDERS - 1) * (STEPS + 1)
STRIDE = 48
WIDE = 256
UNROLL = 4
SMALL = pltpu.CompilerParams(vmem_limit_bytes=8 << 20)
LARGE = pltpu.CompilerParams(vmem_limit_bytes=24 << 20)
PAD = 128
AXES = ("row", "col")
NT = (((1,), (1,)), ((), ()))


def device_count():
    return lax.axis_size("row") * lax.axis_size("col")


def exchange(spread):
    return lax.all_to_all(spread, AXES, 0, 0, tiled=True)


def shifts(axis):
    peers = lax.axis_size(axis)
    up = [(i, i + 1) for i in range(peers - 1)]
    return up, [(j, i) for i, j in up]


def lanes(shape):
    return lax.broadcasted_iota(jnp.int32, shape, len(shape) - 1)


def sublanes(shape):
    return lax.broadcasted_iota(jnp.int32, shape, len(shape) - 2)


def pack_body(before_ref, fields_ref, after_ref, low_ref, high_ref):
    rows, slots, cols = fields_ref.shape
    span = cols // HALO
    lane = lanes((slots, cols))
    edge = HALO // span

    def group(source, shift, g, carry):
        low = jnp.zeros((slots, cols), F32)
        high = jnp.zeros((slots, cols), F32)
        for k in range(span):
            cells = source[(g - shift) * span + k]
            inside = (lane >= k * HALO) & (lane < (k + 1) * HALO)
            first = pltpu.roll(cells, k * HALO, 1) if k else cells
            turn = (k * HALO + HALO) % cols
            second = pltpu.roll(cells, turn, 1) if turn else cells
            low = jnp.where(inside, first, low)
            high = jnp.where(inside, second, high)
        low_ref[g] = low
        high_ref[g] = high
        return carry

    last = edge + rows // span
    lax.fori_loop(0, edge, functools.partial(group, before_ref, 0), 0)
    lax.fori_loop(edge, last, functools.partial(group, fields_ref, edge), 0)
    lax.fori_loop(last, last + edge, functools.partial(group, after_ref, last), 0)


def lower_inverse(matrix, count):
    lane = lanes(matrix.shape)
    row = sublanes(matrix.shape)
    half = PAD // 2
    work = jnp.where(lane < half, matrix, (lane == row + half).astype(F32))
    for j in range(count):
        pivot = work[j : j + 1]
        ratio = work[:, j : j + 1] / work[j : j + 1, j : j + 1]
        work = work - jnp.where(row > j, ratio * pivot, 0.0)
    size = jnp.sum(jnp.where(lane == row, work, 0.0), axis=1, keepdims=True)
    valid = (row < count) & (lane >= half) & (lane < half + count)
    size = jnp.where(sublanes(size.shape) < count, size, 1.0)
    return pltpu.roll(jnp.where(valid, work / jnp.sqrt(size), 0.0), half, 1)


def krylov_body(raw_ref, out_ref):
    groups, length, width = raw_ref.shape
    out_ref[...] = jnp.zeros(out_ref.shape, F32)
    for j in range(groups):
        out_ref[j * K : j * K + length, :width] = raw_ref[j]
    flat = out_ref[...]
    square = lax.dot_general(
        flat, flat, (((0,), (0,)), ((), ())), precision=HIGHEST, preferred_element_type=F32
    )
    inverse = lower_inverse(square[:K], width)
    inverse = jnp.concatenate([inverse, jnp.zeros((PAD - K, PAD), F32)], 0)
    out_ref[...] = lax.dot_general(flat, inverse, NT, precision=HIGHEST, preferred_element_type=F32)


def sideways(main, side, lane):
    cols = main.shape[-1]
    main_up = pltpu.roll(main, 1, 1)
    side_up = pltpu.roll(side, 1, 1)
    main_down = pltpu.roll(main, cols - 1, 1)
    side_down = pltpu.roll(side, cols - 1, 1)
    first = lane == 0
    last = lane == cols - 1
    left = (jnp.where(first, side_up, main_up), jnp.where(first, main_up, side_up))
    right = (jnp.where(last, side_down, main_down), jnp.where(last, main_down, side_down))
    return left, right


def image_body(
    before_ref, fields_ref, after_ref, left_ref, right_ref,
    tall_ref, side_ref, coef_ref, hi_ref, lo_ref, gram_ref,
    local_ref, m1, s1, m2, s2, m3, s3, acc_ref,
):
    total, slots, cols = tall_ref.shape
    rows = total - 2 * HALO
    span = cols // HALO
    lane = lanes((slots, cols))

    def unpack(source, shift, g, carry):
        gathered = [[] for _ in range(8)]
        from_left = left_ref[g]
        from_right = right_ref[g]
        for k in range(span):
            r = g * span + k
            main = source[(g - shift) * span + k]
            tall_ref[r] = main
            turn = (cols - k * HALO) % cols
            low = pltpu.roll(from_right, turn, 1) if turn else from_right
            turn = (cols - HALO - k * HALO) % cols
            high = pltpu.roll(from_left, turn, 1) if turn else from_left
            side = jnp.where(lane < HALO, low, jnp.where(lane >= cols - HALO, high, 0.0))
            packed = []
            for cells in (main, side):
                spin = cells[R + 1 : R + 2]
                couple = COUPLING * cells[R + 2 : R + 3]
                packed += [cells[R : R + 1], spin - couple, -spin - couple, couple]
            local_ref[r] = 2.0 * jnp.concatenate(packed, 0)
            for q in range(8):
                gathered[q].append(packed[q])
            side_ref[r] = side
        for q in range(8):
            coef_ref[q, pl.ds(g * span, span), :] = jnp.concatenate(gathered[q], 0)
        return carry

    first = HALO // span
    last = first + rows // span
    lax.fori_loop(0, first, functools.partial(unpack, before_ref, 0), 0)
    lax.fori_loop(first, last, functools.partial(unpack, fields_ref, first), 0)
    lax.fori_loop(last, last + first, functools.partial(unpack, after_ref, last), 0)

    blank = jnp.zeros((STRIDE - slots, cols), F32)

    def keep(order, r, cells):
        whole = jnp.concatenate([cells, blank], 0)
        high = whole.astype(BF16)
        low = (whole - high.astype(F32)).astype(BF16)
        place = pl.ds(pl.multiple_of((r - HALO) * cols, cols), cols)
        hi_ref[order * STRIDE : (order + 1) * STRIDE, place] = high
        lo_ref[order * STRIDE : (order + 1) * STRIDE, place] = low

    def level(order, source, older, target, need_side):
        source_main, source_side = source

        def one(r, store):
            main = source_main[r]
            side = source_side[r]
            local = local_ref[r]
            left, right = sideways(main, side, lane)
            fresh = (
                local[0:1] * main
                + local[1:2] * right[0]
                + local[2:3] * left[0]
                - local[3:4] * (source_main[r - 1] + source_main[r + 1])
            )
            if order == 1:
                fresh = 0.5 * fresh
            if older is not None:
                fresh = fresh - older[0][r]
            if target is not None:
                target[0][r] = fresh
            if need_side:
                edge = (
                    local[4:5] * side
                    + local[5:6] * right[1]
                    + local[6:7] * left[1]
                    - local[7:8] * (source_side[r - 1] + source_side[r + 1])
                )
                if order == 1:
                    edge = 0.5 * edge
                if older is not None:
                    edge = edge - older[1][r]
                target[1][r] = edge
            if store:
                keep(order, r, fresh)

        reach = ORDERS - 1 - order

        def inner(i, carry):
            for k in range(UNROLL):
                one(HALO + i * UNROLL + k, True)
            return carry

        for k in range(reach):
            one(HALO - 1 - k, False)
            one(HALO + rows + k, False)
        lax.fori_loop(0, rows // UNROLL, inner, 0)

    def plain(i, carry):
        for k in range(UNROLL):
            keep(0, HALO + i * UNROLL + k, tall_ref[HALO + i * UNROLL + k])
        return carry

    lax.fori_loop(0, rows // UNROLL, plain, 0)
    level(1, (tall_ref, side_ref), None, (m1, s1), True)
    level(2, (m1, s1), (tall_ref, side_ref), (m2, s2), True)
    level(3, (m2, s2), (m1, s1), (m3, s3), True)
    level(4, (m3, s3), (m2, s2), None, False)

    size = ORDERS * STRIDE
    chunk = 8 * cols
    acc_ref[...] = jnp.zeros(acc_ref.shape, F32)

    def product(i, carry):
        place = pl.ds(pl.multiple_of(i * chunk, chunk), chunk)
        high = hi_ref[:, place]
        low = lo_ref[:, place]
        acc_ref[:, :size] += (
            lax.dot_general(high, high, NT, preferred_element_type=F32)
            + lax.dot_general(high, low, NT, preferred_element_type=F32)
            + lax.dot_general(low, high, NT, preferred_element_type=F32)
        )
        return carry

    lax.fori_loop(0, rows * cols // chunk, product, 0)
    lane_wide = lanes((K, WIDE))

    def band(order):
        return acc_ref[order * STRIDE : order * STRIDE + K, :]

    bands = [
        band(0),
        jnp.where(lane_wide < STRIDE, pltpu.roll(band(4), WIDE - 4 * STRIDE, 1), band(1)),
        jnp.where(lane_wide < 2 * STRIDE, pltpu.roll(band(3), WIDE - 3 * STRIDE, 1), band(2)),
    ]
    for i in range(3):
        acc_ref[i * K : (i + 1) * K, :] = bands[i]
    count, _, piece = gram_ref.shape
    deep = piece // WIDE
    for i in range(count):
        for k in range(deep):
            gram_ref[i, :, k * WIDE : (k + 1) * WIDE] = acc_ref[i * deep + k : i * deep + k + 1, :]


def relay_body(parts_ref, spread_ref):
    total = jnp.sum(parts_ref[...], axis=0)
    for i in range(spread_ref.shape[0]):
        spread_ref[i] = total


def absorb(parts, state, turn, inverse_total):
    gram, factor, flipped, square, vectors, pending = state
    new_row = R + turn
    column = KRYLOV + turn
    total = jnp.sum(parts, axis=0) * inverse_total
    table = jnp.concatenate(
        [total[:, a * WIDE : (a + 1) * WIDE] for a in range(ORDERS)]
        + [jnp.zeros((8 - ORDERS, WIDE), F32)],
        0,
    )
    lane_one = lanes((1, WIDE))
    norm = jnp.sum(jnp.where(lane_one == new_row, table[0:1], 0.0), axis=1, keepdims=True)
    beta = jnp.sqrt(norm + EPSILON)
    sigma = 1.0 / beta
    here = (lanes((K, PAD)) == new_row) & (sublanes((K, PAD)) == new_row)
    factor = jnp.where(here, sigma, factor)
    flipped = jnp.where(here, sigma, flipped)
    square = jnp.where(here, sigma * sigma, square)
    tall = jnp.transpose(
        jnp.concatenate([table[:, :PAD], jnp.zeros((PAD - 8, PAD), F32)], 0)
    )
    lane_gram = lanes((K, WIDE))
    gram = jnp.where(sublanes((K, WIDE)) == new_row, table[0:1], gram)
    for b in range(ORDERS):
        gram = jnp.where(lane_gram == b * STRIDE + new_row, tall[:K, b : b + 1], gram)

    latest = [vectors[j * K : (j + 1) * K, column - 1 : column] for j in range(4)]
    unit = (lax.broadcasted_iota(jnp.int32, (K, 1), 0) == new_row).astype(F32)
    expanded = jnp.concatenate(
        [
            latest[1],
            0.5 * (latest[0] + latest[2]),
            0.5 * (latest[1] + latest[3]),
            pending + beta * unit,
        ],
        0,
    )
    first = jnp.sum(vectors * expanded, axis=0, keepdims=True)
    ortho = expanded - jnp.sum(vectors * first, axis=1, keepdims=True)
    second = jnp.sum(vectors * ortho, axis=0, keepdims=True)
    ortho = ortho - jnp.sum(vectors * second, axis=1, keepdims=True)
    eta = jnp.sqrt(jnp.sum(ortho * ortho, axis=0, keepdims=True) + EPSILON)
    vectors = jnp.where(lanes((4 * K, PAD)) == column, ortho / eta, vectors)
    hessenberg = first + second + eta * (lanes((1, PAD)) == column).astype(F32)
    return (gram, factor, flipped, square, vectors, pending), table, sigma, hessenberg


def coefficients_of(state, turn):
    gram, factor, flipped, square, vectors, _ = state
    column = KRYLOV + turn
    latest = [vectors[j * K : (j + 1) * K, column - 1 : column] for j in range(4)]
    mixes = [jnp.sum(factor * one, axis=0, keepdims=True) for one in latest]
    wide = [jnp.concatenate([m, jnp.zeros((1, WIDE - PAD), F32)], 1) for m in mixes]
    target = 0.5 * wide[2]
    for j in range(4):
        target = target - pltpu.roll(0.5 * wide[j], (j + 1) * STRIDE, 1)
    raw = jnp.sum(gram * target, axis=1, keepdims=True)
    upper = jnp.sum(square * raw, axis=0, keepdims=True)
    inside = jnp.where(lanes((K, PAD)) < K, gram[:, :PAD], 0.0)
    twice = 2.0 * raw - jnp.sum(inside * upper, axis=1, keepdims=True)
    removed = jnp.sum(square * twice, axis=0, keepdims=True)
    pending = jnp.sum(
        jnp.where(lanes((K, PAD)) == sublanes((K, PAD)), jnp.sum(flipped * twice, axis=0, keepdims=True), 0.0),
        axis=1,
        keepdims=True,
    )
    table = jnp.concatenate(mixes + [removed] + [jnp.zeros((PAD - 5, PAD), F32)], 0)
    return jnp.transpose(table), mixes + [removed], pending


def turn_body(turn, inverse_total, count, *refs):
    refs = list(refs)
    parts_ref = refs.pop(0)
    state_refs = [refs.pop(0) for _ in range(6 if turn else 1)]
    main_ref, side_ref, coef_ref, hi_ref, lo_ref = [refs.pop(0) for _ in range(5)]
    old_fields = [refs.pop(0) for _ in range(turn)]
    old_rows = [refs.pop(0) for _ in range(turn)]
    spread_ref, field_ref, rows_ref, image_ref = [refs.pop(0) for _ in range(4)]
    out_state = [refs.pop(0) for _ in range(6)]
    if turn:
        table_ref, sigma_ref, hessenberg_ref = [refs.pop(0) for _ in range(3)]
    else:
        folded_ref = refs.pop(0)
    z_ref, t_ref = refs

    if turn:
        state = tuple(r[...] for r in state_refs[:5]) + (state_refs[5][:, 0:1],)
        state, table, sigma, hessenberg = absorb(parts_ref[...], state, turn - 1, inverse_total)
        table_ref[...] = table
        sigma_ref[...] = jnp.broadcast_to(sigma, sigma_ref.shape)
        hessenberg_ref[...] = jnp.broadcast_to(hessenberg, hessenberg_ref.shape)
    else:
        pieces, _, piece = parts_ref.shape
        deep = piece // WIDE
        for i in range(pieces):
            for k in range(deep):
                folded_ref[i * deep + k : i * deep + k + 1, :] = (
                    parts_ref[i, :, k * WIDE : (k + 1) * WIDE] * inverse_total
                )
        gram = folded_ref[0:K, :]
        diagonal = lanes((K, PAD)) == sublanes((K, PAD))
        factor = lower_inverse(gram[:, :PAD] + jnp.where(diagonal, GRAM_SHIFT, 0.0), R)
        square = lax.dot_general(
            factor, factor, (((0,), (0,)), ((), ())), precision=HIGHEST, preferred_element_type=F32
        )[:K]
        flipped = jnp.transpose(jnp.concatenate([factor, jnp.zeros((PAD - K, PAD), F32)], 0))[:K]
        state = (gram, factor, flipped, square, state_refs[0][...], None)
    upright, mixes, pending = coefficients_of(state, turn)
    for ref, value in zip(out_state[:5], state[:5]):
        ref[...] = value
    out_state[5][...] = jnp.broadcast_to(pending, out_state[5].shape)

    total, slots, cols = main_ref.shape
    rows = total - 2 * HALO
    raw_only = sublanes((K, cols)) < R
    weights = [jnp.where(raw_only, upright[:K, j : j + 1], 0.0) for j in range(5)]

    def mix(g, carry):
        lists = [[[], []] for _ in range(5)]
        for k in range(8):
            for half, ref in enumerate((main_ref, side_ref)):
                cells = ref[g * 8 + k]
                for j in range(5):
                    lists[j][half].append(jnp.sum(weights[j] * cells, axis=0, keepdims=True))
        for j in range(5):
            for half in range(2):
                z_ref[j, half, pl.ds(pl.multiple_of(g * 8, 8), 8), :] = jnp.concatenate(lists[j][half], 0)
        return carry

    lax.fori_loop(0, total // 8, mix, 0)

    z = []
    for j in range(5):
        pair = [z_ref[j, 0], z_ref[j, 1]]
        for s in range(turn):
            scale = mixes[j][:, R + s : R + s + 1]
            pair = [pair[half] + scale * old_fields[s][half] for half in range(2)]
        z.append(pair)

    lane = lanes((total, cols))
    local = [coef_ref[q] for q in range(8)]

    def operate(pair):
        main, side = pair
        left, right = sideways(main, side, lane)
        out = []
        for half, cells in enumerate(pair):
            c = local[4 * half : 4 * half + 4]
            out.append(
                c[0] * cells
                + c[1] * right[half]
                + c[2] * left[half]
                - c[3] * (pltpu.roll(cells, 1, 0) + pltpu.roll(cells, total - 1, 0))
            )
        return out

    def combine(*terms):
        return [sum(w * p[half] for w, p in terms) for half in range(2)]

    four = z[3]
    three = combine((1.0, z[2]), (2.0, operate(four)))
    two = combine((1.0, z[1]), (2.0, operate(three)), (-1.0, four))
    one = combine((1.0, z[0]), (2.0, operate(two)), (-1.0, three))
    summed = combine((1.0, operate(one)), (-1.0, two))
    field = combine((0.5, z[2]), (-0.5, summed), (-1.0, z[4]))
    field_ref[0] = field[0]
    field_ref[1] = field[1]

    images = [field, operate(field)]
    for _ in range(ORDERS - 2):
        images.append(combine((2.0, operate(images[-1])), (-1.0, images[-2])))
    for a in range(ORDERS):
        t_ref[a] = images[a][0]
    image_ref[...] = t_ref[ORDERS - 1, HALO : HALO + rows, :]
    rows_ref[...] = jnp.zeros(rows_ref.shape, F32)
    for r in range(rows):
        for a in range(ORDERS):
            rows_ref[a : a + 1, r * cols : (r + 1) * cols] = t_ref[a, HALO + r : HALO + r + 1, :]

    size = ORDERS * STRIDE
    chunk = 8 * cols
    table = jnp.zeros((8, size), F32)
    own = jnp.zeros((8, 8 * (turn + 1)), F32)
    for i in range(rows * cols // chunk):
        place = slice(i * chunk, (i + 1) * chunk)
        mine = rows_ref[:, place]
        rounded = mine.astype(BF16).astype(F32)
        both = jnp.concatenate([rounded, mine - rounded], 0).astype(BF16)
        by_high = lax.dot_general(both, hi_ref[:, place], NT, preferred_element_type=F32)
        by_low = lax.dot_general(both, lo_ref[:, place], NT, preferred_element_type=F32)
        table = table + (by_high[0:8] + by_high[8:16] + by_low[0:8])
        others = jnp.concatenate([ref[:, place] for ref in old_rows] + [mine], 0)
        own = own + lax.dot_general(mine, others, NT, precision=HIGHEST, preferred_element_type=F32)
    table = jnp.concatenate([table, jnp.zeros((8, WIDE - size), F32)], 1)
    lane_table = lanes((8, WIDE))
    for s in range(turn + 1):
        for b in range(ORDERS):
            table = jnp.where(
                lane_table == b * STRIDE + R + s, own[:, 8 * s + b : 8 * s + b + 1], table
            )
    flat = jnp.concatenate([table[a : a + 1] for a in range(ORDERS)], 1)
    for i in range(count):
        spread_ref[i] = flat


def final_body(inverse_total, *refs):
    refs = list(refs)
    parts_ref = refs.pop(0)
    state_refs = [refs.pop(0) for _ in range(6)]
    folded_ref = refs.pop(0)
    old_tables = [refs.pop(0) for _ in range(STEPS - 1)]
    old_sigmas = [refs.pop(0) for _ in range(STEPS - 1)]
    old_hessen = [refs.pop(0) for _ in range(STEPS - 1)]
    fields = [refs.pop(0) for _ in range(STEPS)]
    images = [refs.pop(0) for _ in range(STEPS)]
    columns_ref, coefficients_ref, hessenberg_ref, gram_ref, image_ref = refs

    state = tuple(r[...] for r in state_refs[:5]) + (state_refs[5][:, 0:1],)
    state, table, sigma, hessenberg = absorb(parts_ref[...], state, STEPS - 1, inverse_total)
    factor = state[1]
    for j in range(4):
        coefficients_ref[j] = state[4][j * K : (j + 1) * K, :WIDTH]
    hessenberg_ref[...] = jnp.concatenate([r[0:1] for r in old_hessen] + [hessenberg], 0)[:, :WIDTH]
    sigmas = [ref[0:1, 0:1] for ref in old_sigmas] + [sigma]
    rows = columns_ref.shape[1]
    for s in range(STEPS):
        columns_ref[s] = sigmas[s] * fields[s][0, HALO : HALO + rows, :]
        image_ref[s] = sigmas[s] * images[s][...]

    lane_wide = lanes((K, WIDE))
    bands = [folded_ref[i * K : (i + 1) * K, :] for i in range(3)]
    upper = [
        bands[0],
        bands[1],
        bands[2],
        pltpu.roll(bands[2], 3 * STRIDE, 1),
        pltpu.roll(bands[1], 4 * STRIDE, 1),
    ]
    blank = jnp.zeros((STRIDE - K, WIDE), F32)
    stacked = []
    for a in range(ORDERS):
        stacked += [jnp.where((lane_wide >= a * STRIDE) & (lane_wide < ORDERS * STRIDE), upper[a], 0.0), blank]
    whole = jnp.concatenate(stacked + [jnp.zeros((WIDE - ORDERS * STRIDE, WIDE), F32)], 0)
    row_id = sublanes((WIDE, WIDE))
    lane_id = lanes((WIDE, WIDE))
    lower = row_id >= (lane_id // STRIDE + 1) * STRIDE
    whole = jnp.where(lower, jnp.transpose(whole), whole)
    for s, one in enumerate([ref[...] for ref in old_tables] + [table]):
        flipped = jnp.transpose(jnp.concatenate([one, jnp.zeros((PAD - 8, WIDE), F32)], 0))
        for a in range(ORDERS):
            whole = jnp.where(row_id == a * STRIDE + R + s, one[a : a + 1, :], whole)
        for a in range(ORDERS):
            whole = jnp.where(lane_id == a * STRIDE + R + s, flipped[:, a : a + 1], whole)
    padded = jnp.concatenate([factor, jnp.zeros((K, WIDE - PAD), F32)], 1)
    padded = jnp.concatenate([padded, blank], 0)
    blocks = [padded] + [pltpu.roll(padded, a * STRIDE, 1) for a in range(1, ORDERS)]
    diagonal = jnp.concatenate(blocks + [jnp.zeros((WIDE - ORDERS * STRIDE, WIDE), F32)], 0)
    half = jnp.dot(diagonal, whole, precision=HIGHEST, preferred_element_type=F32)
    gram_ref[...] = lax.dot_general(half, diagonal, NT, precision=HIGHEST, preferred_element_type=F32)


def shape(*dims, dtype=F32):
    return jax.ShapeDtypeStruct(dims, dtype)


def local(basis_raw, krylov_raw, stiffness, rotation):
    rows = basis_raw.shape[1]
    cols = basis_raw.shape[2]
    cells = rows * cols
    count = device_count()
    inverse_total = 1.0 / (cells * count)
    total = rows + 2 * HALO
    size = ORDERS * STRIDE

    fields = jnp.concatenate(
        [
            jnp.transpose(basis_raw, (1, 0, 2)),
            stiffness[:, None],
            rotation[:, None],
            jnp.ones((rows, 1, cols), F32),
        ],
        1,
    )
    up, down = shifts("row")
    before = lax.ppermute(fields[rows - HALO :], "row", up)
    after = lax.ppermute(fields[:HALO], "row", down)
    pieces = (before, fields, after)
    strip = shape(total * HALO // cols, K, cols)
    low, high = pl.pallas_call(pack_body, out_shape=(strip, strip), name="pack", compiler_params=SMALL)(*pieces)
    up, down = shifts("col")
    from_left = lax.ppermute(high, "col", up)
    from_right = lax.ppermute(low, "col", down)
    vectors = pl.pallas_call(krylov_body, out_shape=shape(4 * K, PAD), name="krylov", compiler_params=SMALL)(krylov_raw)
    vectors, from_left = lax.optimization_barrier((vectors, from_left))

    level = pltpu.VMEM((total, K, cols), F32)
    piece = PAD * WIDE // count
    tall, side, coefs, hi, lo, folded = pl.pallas_call(
        image_body,
        out_shape=(
            shape(total, K, cols),
            shape(total, K, cols),
            shape(8, total, cols),
            shape(size, cells, dtype=BF16),
            shape(size, cells, dtype=BF16),
            shape(count, 1, piece),
        ),
        scratch_shapes=[pltpu.VMEM((total, 8, cols), F32)]
        + [level] * 6
        + [pltpu.VMEM((size, WIDE), F32)],
        name="images", compiler_params=LARGE,
    )(*pieces, from_left, from_right)

    mine = pl.pallas_call(
        relay_body, out_shape=shape(count, 1, piece), name="relay", compiler_params=SMALL
    )(exchange(folded))
    parts = exchange(mine)

    state_shapes = (
        shape(K, WIDE),
        shape(K, PAD),
        shape(K, PAD),
        shape(K, PAD),
        shape(4 * K, PAD),
        shape(K, PAD),
    )
    state = (vectors,)
    made_fields, made_rows, made_images, tables, sigmas, hessen = [], [], [], [], [], []
    for turn in range(STEPS):
        out_shape = (
            shape(count, 1, ORDERS * WIDE),
            shape(2, total, cols),
            shape(8, cells),
            shape(rows, cols),
        ) + state_shapes
        if turn:
            out_shape += (shape(8, WIDE), shape(8, PAD), shape(8, PAD))
        else:
            out_shape += (shape(PAD, WIDE),)
        outs = pl.pallas_call(
            functools.partial(turn_body, turn, inverse_total, count),
            out_shape=out_shape,
            scratch_shapes=[
                pltpu.VMEM((5, 2, total, cols), F32),
                pltpu.VMEM((ORDERS, total, cols), F32),
            ],
            name=f"turn{turn}", compiler_params=LARGE,
        )(parts, *state, tall, side, coefs, hi, lo, *made_fields, *made_rows)
        made_fields.append(outs[1])
        made_rows.append(outs[2])
        made_images.append(outs[3])
        state = outs[4:10]
        if turn:
            tables.append(outs[10])
            sigmas.append(outs[11])
            hessen.append(outs[12])
        else:
            folded = outs[10]
        parts = exchange(outs[0])

    new_columns, coefficients, hessenberg, gram, new_images = pl.pallas_call(
        functools.partial(final_body, inverse_total),
        out_shape=(
            shape(STEPS, rows, cols),
            shape(4, K, WIDTH),
            shape(STEPS, WIDTH),
            shape(WIDE, WIDE),
            shape(STEPS, rows, cols),
        ),
        name="final", compiler_params=SMALL,
    )(parts, *state, folded, *tables, *sigmas, *hessen, *made_fields, *made_images)
    gram = gram[:size, :size].reshape(ORDERS, STRIDE, ORDERS, STRIDE)[:, :K, :, :K]
    return (new_columns, coefficients, hessenberg, gram, new_images)


def solution(mesh):
    in_specs = (P(None, "row", "col"), P(), P("row", "col"), P("row", "col"))
    out_specs = (P(None, "row", "col"), P(), P(), P(), P(None, "row", "col"))
    return jax.shard_map(local, mesh=mesh, in_specs=in_specs, out_specs=out_specs, check_vma=False)
```

```python
import functools
import jax
import jax.numpy as jnp
from jax import lax
from jax.experimental import pallas as pl
from jax.experimental.pallas import tpu as pltpu
from jax.sharding import PartitionSpec as P

K = 40
STEPS = 3
R = 37
KRYLOV = 34
WIDTH = KRYLOV + STEPS

COUPLING = 0.2
EPSILON = 1e-06
GRAM_SHIFT = 0.05
HIGHEST = lax.Precision.HIGHEST
F32 = jnp.float32
BF16 = jnp.bfloat16

ORDERS = 5
HALO = (ORDERS - 1) * (STEPS + 1)
STRIDE = 48
WIDE = 256
UNROLL = 4
SMALL = pltpu.CompilerParams(vmem_limit_bytes=8 << 20)
LARGE = pltpu.CompilerParams(vmem_limit_bytes=24 << 20)
PAD = 128
AXES = ("row", "col")
NT = (((1,), (1,)), ((), ()))


def device_count():
    return lax.axis_size("row") * lax.axis_size("col")


def exchange(spread):
    return lax.all_to_all(spread, AXES, 0, 0, tiled=True)


def shifts(axis):
    peers = lax.axis_size(axis)
    up = [(i, i + 1) for i in range(peers - 1)]
    return up, [(j, i) for i, j in up]


def lanes(shape):
    return lax.broadcasted_iota(jnp.int32, shape, len(shape) - 1)


def sublanes(shape):
    return lax.broadcasted_iota(jnp.int32, shape, len(shape) - 2)


def pack_body(before_ref, fields_ref, after_ref, low_ref, high_ref):
    rows, slots, cols = fields_ref.shape
    span = cols // HALO
    lane = lanes((slots, cols))
    edge = HALO // span

    def group(source, shift, g, carry):
        low = jnp.zeros((slots, cols), F32)
        high = jnp.zeros((slots, cols), F32)
        for k in range(span):
            cells = source[(g - shift) * span + k]
            inside = (lane >= k * HALO) & (lane < (k + 1) * HALO)
            first = pltpu.roll(cells, k * HALO, 1) if k else cells
            turn = (k * HALO + HALO) % cols
            second = pltpu.roll(cells, turn, 1) if turn else cells
            low = jnp.where(inside, first, low)
            high = jnp.where(inside, second, high)
        low_ref[g] = low
        high_ref[g] = high
        return carry

    last = edge + rows // span
    lax.fori_loop(0, edge, functools.partial(group, before_ref, 0), 0)
    lax.fori_loop(edge, last, functools.partial(group, fields_ref, edge), 0)
    lax.fori_loop(last, last + edge, functools.partial(group, after_ref, last), 0)


def lower_inverse(matrix, count):
    half = PAD // 2
    block = 4
    tile = (8, PAD)
    groups = range(K // 8)
    lane = lanes(tile)
    row = [sublanes(tile) + 8 * g for g in groups]
    work = []
    for g in groups:
        used = (row[g] < count) & (lane < count)
        left = jnp.where(used, matrix[8 * g : 8 * g + 8], (lane == row[g]).astype(F32))
        work.append(jnp.where(lane < half, left, (lane == row[g] + half).astype(F32)))
    for start in range(0, K, block):
        active = [g for g in groups if 8 * g + 7 > start]
        spots = range(start, start + block)
        pivots = [jnp.broadcast_to(work[j // 8][j % 8 : j % 8 + 1], tile) for j in spots]
        below = [
            {g: jnp.broadcast_to(work[g][:, j : j + 1], tile) for g in active} for j in spots
        ]
        corner = [
            [jnp.broadcast_to(pivots[i][:, j : j + 1], tile) for j in spots] for i in range(block)
        ]
        for i in range(block):
            inverse = 1.0 / corner[i][i]
            for k in range(i + 1, block):
                ratio = corner[i][k] * inverse
                pivots[k] = pivots[k] - pivots[i] * ratio
                for g in active:
                    below[k][g] = below[k][g] - below[i][g] * ratio
                for other in range(k, block):
                    corner[k][other] = corner[k][other] - corner[i][other] * ratio
            below[i] = {g: below[i][g] * inverse for g in active}
        for g in active:
            for i in range(block):
                work[g] = work[g] - jnp.where(row[g] > start + i, below[i][g] * pivots[i], 0.0)
    out = []
    for g in groups:
        size = jnp.sum(jnp.where(lane == row[g], work[g], 0.0), axis=1, keepdims=True)
        valid = (row[g] < count) & (lane >= half) & (lane < half + count)
        out.append(pltpu.roll(jnp.where(valid, work[g] / jnp.sqrt(size), 0.0), half, 1))
    return jnp.concatenate(out, 0)


def krylov_body(raw_ref, out_ref):
    groups, length, width = raw_ref.shape
    out_ref[...] = jnp.zeros(out_ref.shape, F32)
    for j in range(groups):
        out_ref[j * K : j * K + length, :width] = raw_ref[j]
    flat = out_ref[...]
    square = lax.dot_general(
        flat, flat, (((0,), (0,)), ((), ())), precision=HIGHEST, preferred_element_type=F32
    )
    inverse = lower_inverse(square[:K], width)
    inverse = jnp.concatenate([inverse, jnp.zeros((PAD - K, PAD), F32)], 0)
    out_ref[...] = lax.dot_general(flat, inverse, NT, precision=HIGHEST, preferred_element_type=F32)


def sideways(main, side, lane):
    cols = main.shape[-1]
    main_up = pltpu.roll(main, 1, 1)
    side_up = pltpu.roll(side, 1, 1)
    main_down = pltpu.roll(main, cols - 1, 1)
    side_down = pltpu.roll(side, cols - 1, 1)
    first = lane == 0
    last = lane == cols - 1
    left = (jnp.where(first, side_up, main_up), jnp.where(first, main_up, side_up))
    right = (jnp.where(last, side_down, main_down), jnp.where(last, main_down, side_down))
    return left, right


def image_body(
    before_ref, fields_ref, after_ref, left_ref, right_ref,
    tall_ref, side_ref, coef_ref, split_ref, gram_ref,
    local_ref, m1, s1, m2, s2, m3, s3, acc_ref,
):
    total, slots, cols = tall_ref.shape
    rows = total - 2 * HALO
    span = cols // HALO
    lane = lanes((slots, cols))

    def unpack(source, shift, g, carry):
        gathered = [[] for _ in range(8)]
        from_left = left_ref[g]
        from_right = right_ref[g]
        for k in range(span):
            r = g * span + k
            main = source[(g - shift) * span + k]
            tall_ref[r] = main
            turn = (cols - k * HALO) % cols
            low = pltpu.roll(from_right, turn, 1) if turn else from_right
            turn = (cols - HALO - k * HALO) % cols
            high = pltpu.roll(from_left, turn, 1) if turn else from_left
            side = jnp.where(lane < HALO, low, jnp.where(lane >= cols - HALO, high, 0.0))
            packed = []
            for cells in (main, side):
                spin = cells[R + 1 : R + 2]
                couple = COUPLING * cells[R + 2 : R + 3]
                packed += [cells[R : R + 1], spin - couple, -spin - couple, couple]
            local_ref[r] = 2.0 * jnp.concatenate(packed, 0)
            for q in range(8):
                gathered[q].append(packed[q])
            side_ref[r] = side
        for q in range(8):
            coef_ref[q, pl.ds(g * span, span), :] = jnp.concatenate(gathered[q], 0)
        return carry

    first = HALO // span
    last = first + rows // span
    lax.fori_loop(0, first, functools.partial(unpack, before_ref, 0), 0)
    lax.fori_loop(first, last, functools.partial(unpack, fields_ref, first), 0)
    lax.fori_loop(last, last + first, functools.partial(unpack, after_ref, last), 0)

    blank = jnp.zeros((STRIDE - slots, cols), F32)
    size = ORDERS * STRIDE

    def keep(order, r, cells):
        whole = jnp.concatenate([cells, blank], 0)
        high = whole.astype(BF16)
        low = (whole - high.astype(F32)).astype(BF16)
        place = pl.ds(pl.multiple_of((r - HALO) * cols, cols), cols)
        split_ref[order * STRIDE : (order + 1) * STRIDE, place] = high
        split_ref[size + order * STRIDE : size + (order + 1) * STRIDE, place] = low

    def level(order, source, older, target, need_side):
        source_main, source_side = source

        def one(r, store):
            main = source_main[r]
            side = source_side[r]
            local = local_ref[r]
            left, right = sideways(main, side, lane)
            fresh = (
                local[0:1] * main
                + local[1:2] * right[0]
                + local[2:3] * left[0]
                - local[3:4] * (source_main[r - 1] + source_main[r + 1])
            )
            if order == 1:
                fresh = 0.5 * fresh
            if older is not None:
                fresh = fresh - older[0][r]
            if target is not None:
                target[0][r] = fresh
            if need_side:
                edge = (
                    local[4:5] * side
                    + local[5:6] * right[1]
                    + local[6:7] * left[1]
                    - local[7:8] * (source_side[r - 1] + source_side[r + 1])
                )
                if order == 1:
                    edge = 0.5 * edge
                if older is not None:
                    edge = edge - older[1][r]
                target[1][r] = edge
            if store:
                keep(order, r, fresh)

        reach = ORDERS - 1 - order

        def inner(i, carry):
            for k in range(UNROLL):
                one(HALO + i * UNROLL + k, True)
            return carry

        for k in range(reach):
            one(HALO - 1 - k, False)
            one(HALO + rows + k, False)
        lax.fori_loop(0, rows // UNROLL, inner, 0)

    def plain(i, carry):
        for k in range(UNROLL):
            keep(0, HALO + i * UNROLL + k, tall_ref[HALO + i * UNROLL + k])
        return carry

    lax.fori_loop(0, rows // UNROLL, plain, 0)
    level(1, (tall_ref, side_ref), None, (m1, s1), True)
    level(2, (m1, s1), (tall_ref, side_ref), (m2, s2), True)
    level(3, (m2, s2), (m1, s1), (m3, s3), True)
    level(4, (m3, s3), (m2, s2), None, False)

    chunk = rows * cols // 3
    for i in range(3):
        place = slice(i * chunk, (i + 1) * chunk)
        part = lax.dot_general(
            split_ref[:, place], split_ref[:size, place], NT, preferred_element_type=F32
        )
        if i:
            acc_ref[:, :size] += part
        else:
            acc_ref[:, :size] = part
    cross = jnp.concatenate(
        [acc_ref[size:, :size], jnp.zeros((size, WIDE - size), F32)], 1
    )
    cross = jnp.concatenate([cross, jnp.zeros((WIDE - size, WIDE), F32)], 0)
    acc_ref[:size, :size] += (cross + jnp.transpose(cross))[:size, :size]
    lane_wide = lanes((K, WIDE))

    def band(order):
        return acc_ref[order * STRIDE : order * STRIDE + K, :]

    bands = [
        band(0),
        jnp.where(lane_wide < STRIDE, pltpu.roll(band(4), WIDE - 4 * STRIDE, 1), band(1)),
        jnp.where(lane_wide < 2 * STRIDE, pltpu.roll(band(3), WIDE - 3 * STRIDE, 1), band(2)),
    ]
    for i in range(3):
        acc_ref[i * K : (i + 1) * K, :] = bands[i]
    count, _, piece = gram_ref.shape
    deep = piece // WIDE
    for i in range(count):
        for k in range(deep):
            gram_ref[i, :, k * WIDE : (k + 1) * WIDE] = acc_ref[i * deep + k : i * deep + k + 1, :]


def relay_body(parts_ref, spread_ref):
    total = jnp.sum(parts_ref[...], axis=0)
    for i in range(spread_ref.shape[0]):
        spread_ref[i] = total


def absorb(parts, state, turn, inverse_total):
    gram, factor, flipped, square, vectors, pending = state
    new_row = R + turn
    column = KRYLOV + turn
    total = jnp.sum(parts, axis=0) * inverse_total
    table = jnp.concatenate(
        [total[:, a * WIDE : (a + 1) * WIDE] for a in range(ORDERS)]
        + [jnp.zeros((8 - ORDERS, WIDE), F32)],
        0,
    )
    lane_one = lanes((1, WIDE))
    norm = jnp.sum(jnp.where(lane_one == new_row, table[0:1], 0.0), axis=1, keepdims=True)
    beta = jnp.sqrt(norm + EPSILON)
    sigma = 1.0 / beta
    here = (lanes((K, PAD)) == new_row) & (sublanes((K, PAD)) == new_row)
    factor = jnp.where(here, sigma, factor)
    flipped = jnp.where(here, sigma, flipped)
    square = jnp.where(here, sigma * sigma, square)
    tall = jnp.transpose(
        jnp.concatenate([table[:, :PAD], jnp.zeros((PAD - 8, PAD), F32)], 0)
    )
    lane_gram = lanes((K, WIDE))
    gram = jnp.where(sublanes((K, WIDE)) == new_row, table[0:1], gram)
    for b in range(ORDERS):
        gram = jnp.where(lane_gram == b * STRIDE + new_row, tall[:K, b : b + 1], gram)

    latest = [vectors[j * K : (j + 1) * K, column - 1 : column] for j in range(4)]
    unit = (lax.broadcasted_iota(jnp.int32, (K, 1), 0) == new_row).astype(F32)
    expanded = jnp.concatenate(
        [
            latest[1],
            0.5 * (latest[0] + latest[2]),
            0.5 * (latest[1] + latest[3]),
            pending + beta * unit,
        ],
        0,
    )
    first = jnp.sum(vectors * expanded, axis=0, keepdims=True)
    ortho = expanded - jnp.sum(vectors * first, axis=1, keepdims=True)
    second = jnp.sum(vectors * ortho, axis=0, keepdims=True)
    ortho = ortho - jnp.sum(vectors * second, axis=1, keepdims=True)
    eta = jnp.sqrt(jnp.sum(ortho * ortho, axis=0, keepdims=True) + EPSILON)
    vectors = jnp.where(lanes((4 * K, PAD)) == column, ortho / eta, vectors)
    hessenberg = first + second + eta * (lanes((1, PAD)) == column).astype(F32)
    return (gram, factor, flipped, square, vectors, pending), table, sigma, hessenberg


def coefficients_of(state, turn):
    gram, factor, flipped, square, vectors, _ = state
    column = KRYLOV + turn
    latest = [vectors[j * K : (j + 1) * K, column - 1 : column] for j in range(4)]
    mixes = [jnp.sum(factor * one, axis=0, keepdims=True) for one in latest]
    wide = [jnp.concatenate([m, jnp.zeros((1, WIDE - PAD), F32)], 1) for m in mixes]
    target = 0.5 * wide[2]
    for j in range(4):
        target = target - pltpu.roll(0.5 * wide[j], (j + 1) * STRIDE, 1)
    raw = jnp.sum(gram * target, axis=1, keepdims=True)
    upper = jnp.sum(square * raw, axis=0, keepdims=True)
    inside = jnp.where(lanes((K, PAD)) < K, gram[:, :PAD], 0.0)
    twice = 2.0 * raw - jnp.sum(inside * upper, axis=1, keepdims=True)
    removed = jnp.sum(square * twice, axis=0, keepdims=True)
    pending = jnp.sum(
        jnp.where(lanes((K, PAD)) == sublanes((K, PAD)), jnp.sum(flipped * twice, axis=0, keepdims=True), 0.0),
        axis=1,
        keepdims=True,
    )
    table = jnp.concatenate(mixes + [removed] + [jnp.zeros((PAD - 5, PAD), F32)], 0)
    return jnp.transpose(table), mixes + [removed], pending


def turn_body(turn, inverse_total, count, *refs):
    refs = list(refs)
    parts_ref = refs.pop(0)
    state_refs = [refs.pop(0) for _ in range(6 if turn else 1)]
    main_ref, side_ref, coef_ref, split_ref = [refs.pop(0) for _ in range(4)]
    old_fields = [refs.pop(0) for _ in range(turn)]
    old_rows = [refs.pop(0) for _ in range(turn)]
    spread_ref, field_ref, rows_ref, image_ref = [refs.pop(0) for _ in range(4)]
    out_state = [refs.pop(0) for _ in range(6)]
    if turn:
        table_ref, sigma_ref, hessenberg_ref = [refs.pop(0) for _ in range(3)]
    else:
        folded_ref = refs.pop(0)
    z_ref, t_ref, flat_ref = refs

    if turn:
        state = tuple(r[...] for r in state_refs[:5]) + (state_refs[5][:, 0:1],)
        state, table, sigma, hessenberg = absorb(parts_ref[...], state, turn - 1, inverse_total)
        table_ref[...] = table
        sigma_ref[...] = jnp.broadcast_to(sigma, sigma_ref.shape)
        hessenberg_ref[...] = jnp.broadcast_to(hessenberg, hessenberg_ref.shape)
    else:
        pieces, _, piece = parts_ref.shape
        deep = piece // WIDE
        for i in range(pieces):
            for k in range(deep):
                folded_ref[i * deep + k : i * deep + k + 1, :] = (
                    parts_ref[i, :, k * WIDE : (k + 1) * WIDE] * inverse_total
                )
        gram = folded_ref[0:K, :]
        diagonal = lanes((K, PAD)) == sublanes((K, PAD))
        factor = lower_inverse(gram[:, :PAD] + jnp.where(diagonal, GRAM_SHIFT, 0.0), R)
        square = lax.dot_general(
            factor, factor, (((0,), (0,)), ((), ())), precision=HIGHEST, preferred_element_type=F32
        )[:K]
        flipped = jnp.transpose(jnp.concatenate([factor, jnp.zeros((PAD - K, PAD), F32)], 0))[:K]
        state = (gram, factor, flipped, square, state_refs[0][...], None)
    upright, mixes, pending = coefficients_of(state, turn)
    for ref, value in zip(out_state[:5], state[:5]):
        ref[...] = value
    out_state[5][...] = jnp.broadcast_to(pending, out_state[5].shape)

    total, slots, cols = main_ref.shape
    rows = total - 2 * HALO
    raw_only = sublanes((K, cols)) < R
    weights = [jnp.where(raw_only, upright[:K, j : j + 1], 0.0) for j in range(5)]

    def mix(g, carry):
        lists = [[[], []] for _ in range(5)]
        for k in range(8):
            for half, ref in enumerate((main_ref, side_ref)):
                cells = ref[g * 8 + k]
                for j in range(5):
                    lists[j][half].append(jnp.sum(weights[j] * cells, axis=0, keepdims=True))
        for j in range(5):
            for half in range(2):
                z_ref[j, half, pl.ds(pl.multiple_of(g * 8, 8), 8), :] = jnp.concatenate(lists[j][half], 0)
        return carry

    lax.fori_loop(0, total // 8, mix, 0)

    z = []
    for j in range(5):
        pair = [z_ref[j, 0], z_ref[j, 1]]
        for s in range(turn):
            scale = mixes[j][:, R + s : R + s + 1]
            pair = [pair[half] + scale * old_fields[s][half] for half in range(2)]
        z.append(pair)

    lane = lanes((total, cols))
    local = [coef_ref[q] for q in range(8)]

    def operate(pair):
        main, side = pair
        left, right = sideways(main, side, lane)
        out = []
        for half, cells in enumerate(pair):
            c = local[4 * half : 4 * half + 4]
            out.append(
                c[0] * cells
                + c[1] * right[half]
                + c[2] * left[half]
                - c[3] * (pltpu.roll(cells, 1, 0) + pltpu.roll(cells, total - 1, 0))
            )
        return out

    def combine(*terms):
        return [sum(w * p[half] for w, p in terms) for half in range(2)]

    four = z[3]
    three = combine((1.0, z[2]), (2.0, operate(four)))
    two = combine((1.0, z[1]), (2.0, operate(three)), (-1.0, four))
    one = combine((1.0, z[0]), (2.0, operate(two)), (-1.0, three))
    summed = combine((1.0, operate(one)), (-1.0, two))
    field = combine((0.5, z[2]), (-0.5, summed), (-1.0, z[4]))
    field_ref[0] = field[0]
    field_ref[1] = field[1]

    images = [field, operate(field)]
    for _ in range(ORDERS - 2):
        images.append(combine((2.0, operate(images[-1])), (-1.0, images[-2])))
    for a in range(ORDERS):
        t_ref[a] = images[a][0]
    image_ref[...] = t_ref[ORDERS - 1, HALO : HALO + rows, :]
    t_ref[ORDERS:] = jnp.zeros((8 - ORDERS, total, cols), F32)
    for r in range(rows):
        flat_ref[:, r * cols : (r + 1) * cols] = t_ref[:, HALO + r, :]

    size = ORDERS * STRIDE
    chunk = rows * cols // 3
    table = jnp.zeros((2 * size, 16), F32)
    own = jnp.zeros((16, 16 * (turn + 1)), F32)
    for i in range(3):
        place = slice(i * chunk, (i + 1) * chunk)
        mine = flat_ref[:, place]
        rounded = mine.astype(BF16).astype(F32)
        both = jnp.concatenate([rounded, mine - rounded], 0).astype(BF16)
        rows_ref[:, place] = both
        table = table + lax.dot_general(
            split_ref[:, place], both, NT, preferred_element_type=F32
        )
        others = jnp.concatenate([ref[:, place] for ref in old_rows] + [both], 0)
        own = own + lax.dot_general(both, others, NT, preferred_element_type=F32)
    own = [
        own[0:8, 16 * s : 16 * s + 8]
        + own[0:8, 16 * s + 8 : 16 * s + 16]
        + own[8:16, 16 * s : 16 * s + 8]
        for s in range(turn + 1)
    ]
    table = table[:size, 0:8] + table[:size, 8:16] + table[size:, 0:8]
    table = jnp.concatenate([table, jnp.zeros((size, PAD - 8), F32)], 1)
    table = jnp.transpose(jnp.concatenate([table, jnp.zeros((WIDE - size, PAD), F32)], 0))[:8]
    lane_table = lanes((8, WIDE))
    for s in range(turn + 1):
        for b in range(ORDERS):
            table = jnp.where(
                lane_table == b * STRIDE + R + s, own[s][:, b : b + 1], table
            )
    flat = jnp.concatenate([table[a : a + 1] for a in range(ORDERS)], 1)
    for i in range(count):
        spread_ref[i] = flat


def final_body(inverse_total, *refs):
    refs = list(refs)
    parts_ref = refs.pop(0)
    state_refs = [refs.pop(0) for _ in range(6)]
    folded_ref = refs.pop(0)
    old_tables = [refs.pop(0) for _ in range(STEPS - 1)]
    old_sigmas = [refs.pop(0) for _ in range(STEPS - 1)]
    old_hessen = [refs.pop(0) for _ in range(STEPS - 1)]
    fields = [refs.pop(0) for _ in range(STEPS)]
    images = [refs.pop(0) for _ in range(STEPS)]
    columns_ref, coefficients_ref, hessenberg_ref, gram_ref, image_ref = refs

    state = tuple(r[...] for r in state_refs[:5]) + (state_refs[5][:, 0:1],)
    state, table, sigma, hessenberg = absorb(parts_ref[...], state, STEPS - 1, inverse_total)
    factor = state[1]
    for j in range(4):
        coefficients_ref[j] = state[4][j * K : (j + 1) * K, :WIDTH]
    hessenberg_ref[...] = jnp.concatenate([r[0:1] for r in old_hessen] + [hessenberg], 0)[:, :WIDTH]
    sigmas = [ref[0:1, 0:1] for ref in old_sigmas] + [sigma]
    rows = columns_ref.shape[1]
    for s in range(STEPS):
        columns_ref[s] = sigmas[s] * fields[s][0, HALO : HALO + rows, :]
        image_ref[s] = sigmas[s] * images[s][...]

    lane_wide = lanes((K, WIDE))
    bands = [folded_ref[i * K : (i + 1) * K, :] for i in range(3)]
    upper = [
        bands[0],
        bands[1],
        bands[2],
        pltpu.roll(bands[2], 3 * STRIDE, 1),
        pltpu.roll(bands[1], 4 * STRIDE, 1),
    ]
    blank = jnp.zeros((STRIDE - K, WIDE), F32)
    stacked = []
    for a in range(ORDERS):
        stacked += [jnp.where((lane_wide >= a * STRIDE) & (lane_wide < ORDERS * STRIDE), upper[a], 0.0), blank]
    whole = jnp.concatenate(stacked + [jnp.zeros((WIDE - ORDERS * STRIDE, WIDE), F32)], 0)
    row_id = sublanes((WIDE, WIDE))
    lane_id = lanes((WIDE, WIDE))
    lower = row_id >= (lane_id // STRIDE + 1) * STRIDE
    whole = jnp.where(lower, jnp.transpose(whole), whole)
    for s, one in enumerate([ref[...] for ref in old_tables] + [table]):
        flipped = jnp.transpose(jnp.concatenate([one, jnp.zeros((PAD - 8, WIDE), F32)], 0))
        for a in range(ORDERS):
            whole = jnp.where(row_id == a * STRIDE + R + s, one[a : a + 1, :], whole)
        for a in range(ORDERS):
            whole = jnp.where(lane_id == a * STRIDE + R + s, flipped[:, a : a + 1], whole)
    padded = jnp.concatenate([factor, jnp.zeros((K, WIDE - PAD), F32)], 1)
    padded = jnp.concatenate([padded, blank], 0)
    blocks = [padded] + [pltpu.roll(padded, a * STRIDE, 1) for a in range(1, ORDERS)]
    diagonal = jnp.concatenate(blocks + [jnp.zeros((WIDE - ORDERS * STRIDE, WIDE), F32)], 0)
    half = jnp.dot(diagonal, whole, precision=HIGHEST, preferred_element_type=F32)
    gram_ref[...] = lax.dot_general(half, diagonal, NT, precision=HIGHEST, preferred_element_type=F32)


def shape(*dims, dtype=F32):
    return jax.ShapeDtypeStruct(dims, dtype)


def local(basis_raw, krylov_raw, stiffness, rotation):
    rows = basis_raw.shape[1]
    cols = basis_raw.shape[2]
    cells = rows * cols
    count = device_count()
    inverse_total = 1.0 / (cells * count)
    total = rows + 2 * HALO
    size = ORDERS * STRIDE

    fields = jnp.concatenate(
        [
            jnp.transpose(basis_raw, (1, 0, 2)),
            stiffness[:, None],
            rotation[:, None],
            jnp.ones((rows, 1, cols), F32),
        ],
        1,
    )
    up, down = shifts("row")
    before = lax.ppermute(fields[rows - HALO :], "row", up)
    after = lax.ppermute(fields[:HALO], "row", down)
    pieces = (before, fields, after)
    strip = shape(total * HALO // cols, K, cols)
    low, high = pl.pallas_call(pack_body, out_shape=(strip, strip), name="pack", compiler_params=SMALL)(*pieces)
    up, down = shifts("col")
    from_left = lax.ppermute(high, "col", up)
    from_right = lax.ppermute(low, "col", down)
    vectors = pl.pallas_call(krylov_body, out_shape=shape(4 * K, PAD), name="krylov", compiler_params=SMALL)(krylov_raw)
    vectors, from_left = lax.optimization_barrier((vectors, from_left))

    level = pltpu.VMEM((total, K, cols), F32)
    piece = PAD * WIDE // count
    tall, side, coefs, split, folded = pl.pallas_call(
        image_body,
        out_shape=(
            shape(total, K, cols),
            shape(total, K, cols),
            shape(8, total, cols),
            shape(2 * size, cells, dtype=BF16),
            shape(count, 1, piece),
        ),
        scratch_shapes=[pltpu.VMEM((total, 8, cols), F32)]
        + [level] * 6
        + [pltpu.VMEM((2 * size, WIDE), F32)],
        name="images", compiler_params=LARGE,
    )(*pieces, from_left, from_right)

    mine = pl.pallas_call(
        relay_body, out_shape=shape(count, 1, piece), name="relay", compiler_params=SMALL
    )(exchange(folded))
    parts = exchange(mine)

    state_shapes = (
        shape(K, WIDE),
        shape(K, PAD),
        shape(K, PAD),
        shape(K, PAD),
        shape(4 * K, PAD),
        shape(K, PAD),
    )
    state = (vectors,)
    made_fields, made_rows, made_images, tables, sigmas, hessen = [], [], [], [], [], []
    for turn in range(STEPS):
        out_shape = (
            shape(count, 1, ORDERS * WIDE),
            shape(2, total, cols),
            shape(16, cells, dtype=BF16),
            shape(rows, cols),
        ) + state_shapes
        if turn:
            out_shape += (shape(8, WIDE), shape(8, PAD), shape(8, PAD))
        else:
            out_shape += (shape(PAD, WIDE),)
        outs = pl.pallas_call(
            functools.partial(turn_body, turn, inverse_total, count),
            out_shape=out_shape,
            scratch_shapes=[
                pltpu.VMEM((5, 2, total, cols), F32),
                pltpu.VMEM((8, total, cols), F32),
                pltpu.VMEM((8, cells), F32),
            ],
            name=f"turn{turn}", compiler_params=LARGE,
        )(parts, *state, tall, side, coefs, split, *made_fields, *made_rows)
        made_fields.append(outs[1])
        made_rows.append(outs[2])
        made_images.append(outs[3])
        state = outs[4:10]
        if turn:
            tables.append(outs[10])
            sigmas.append(outs[11])
            hessen.append(outs[12])
        else:
            folded = outs[10]
        parts = exchange(outs[0])

    new_columns, coefficients, hessenberg, gram, new_images = pl.pallas_call(
        functools.partial(final_body, inverse_total),
        out_shape=(
            shape(STEPS, rows, cols),
            shape(4, K, WIDTH),
            shape(STEPS, WIDTH),
            shape(WIDE, WIDE),
            shape(STEPS, rows, cols),
        ),
        name="final", compiler_params=SMALL,
    )(parts, *state, folded, *tables, *sigmas, *hessen, *made_fields, *made_images)
    gram = gram[:size, :size].reshape(ORDERS, STRIDE, ORDERS, STRIDE)[:, :K, :, :K]
    return (new_columns, coefficients, hessenberg, gram, new_images)


def solution(mesh):
    in_specs = (P(None, "row", "col"), P(), P("row", "col"), P("row", "col"))
    out_specs = (P(None, "row", "col"), P(), P(), P(), P(None, "row", "col"))
    return jax.shard_map(local, mesh=mesh, in_specs=in_specs, out_specs=out_specs, check_vma=False)
```

```python
import functools
import jax
import jax.numpy as jnp
from jax import lax
from jax.experimental import pallas as pl
from jax.experimental.pallas import tpu as pltpu
from jax.sharding import PartitionSpec as P

K = 40
STEPS = 3
R = 37
KRYLOV = 34
WIDTH = KRYLOV + STEPS

COUPLING = 0.2
EPSILON = 1e-06
GRAM_SHIFT = 0.05
HIGHEST = lax.Precision.HIGHEST
F32 = jnp.float32
BF16 = jnp.bfloat16

ORDERS = 5
HALO = (ORDERS - 1) * (STEPS + 1)
STRIDE = 48
WIDE = 256
UNROLL = 24
GROUPS = 2
SMALL = pltpu.CompilerParams(vmem_limit_bytes=8 << 20)
LARGE = pltpu.CompilerParams(vmem_limit_bytes=24 << 20)
PAD = 128
AXES = ("row", "col")
NT = (((1,), (1,)), ((), ()))


def device_count():
    return lax.axis_size("row") * lax.axis_size("col")


def exchange(spread):
    return lax.all_to_all(spread, AXES, 0, 0, tiled=True)


def shifts(axis):
    peers = lax.axis_size(axis)
    up = [(i, i + 1) for i in range(peers - 1)]
    return up, [(j, i) for i, j in up]


def lanes(shape):
    return lax.broadcasted_iota(jnp.int32, shape, len(shape) - 1)


def sublanes(shape):
    return lax.broadcasted_iota(jnp.int32, shape, len(shape) - 2)


def pack_body(before_ref, fields_ref, after_ref, low_ref, high_ref):
    rows, slots, cols = fields_ref.shape
    span = cols // HALO
    lane = lanes((slots, cols))
    edge = HALO // span

    def group(source, shift, g, carry):
        low = jnp.zeros((slots, cols), F32)
        high = jnp.zeros((slots, cols), F32)
        for k in range(span):
            cells = source[(g - shift) * span + k]
            inside = (lane >= k * HALO) & (lane < (k + 1) * HALO)
            first = pltpu.roll(cells, k * HALO, 1) if k else cells
            turn = (k * HALO + HALO) % cols
            second = pltpu.roll(cells, turn, 1) if turn else cells
            low = jnp.where(inside, first, low)
            high = jnp.where(inside, second, high)
        low_ref[g] = low
        high_ref[g] = high
        return carry

    last = edge + rows // span
    lax.fori_loop(0, edge, functools.partial(group, before_ref, 0), 0)
    lax.fori_loop(edge, last, functools.partial(group, fields_ref, edge), 0)
    lax.fori_loop(last, last + edge, functools.partial(group, after_ref, last), 0)


def lower_inverse(matrix, count):
    half = PAD // 2
    block = 4
    tile = (8, PAD)
    groups = range(K // 8)
    lane = lanes(tile)
    row = [sublanes(tile) + 8 * g for g in groups]
    work = []
    for g in groups:
        used = (row[g] < count) & (lane < count)
        left = jnp.where(used, matrix[8 * g : 8 * g + 8], (lane == row[g]).astype(F32))
        work.append(jnp.where(lane < half, left, (lane == row[g] + half).astype(F32)))
    for start in range(0, K, block):
        active = [g for g in groups if 8 * g + 7 > start]
        spots = range(start, start + block)
        pivots = [jnp.broadcast_to(work[j // 8][j % 8 : j % 8 + 1], tile) for j in spots]
        below = [
            {g: jnp.broadcast_to(work[g][:, j : j + 1], tile) for g in active} for j in spots
        ]
        corner = [
            [jnp.broadcast_to(pivots[i][:, j : j + 1], tile) for j in spots] for i in range(block)
        ]
        for i in range(block):
            inverse = 1.0 / corner[i][i]
            for k in range(i + 1, block):
                ratio = corner[i][k] * inverse
                pivots[k] = pivots[k] - pivots[i] * ratio
                for g in active:
                    below[k][g] = below[k][g] - below[i][g] * ratio
                for other in range(k, block):
                    corner[k][other] = corner[k][other] - corner[i][other] * ratio
            below[i] = {g: below[i][g] * inverse for g in active}
        for g in active:
            for i in range(block):
                work[g] = work[g] - jnp.where(row[g] > start + i, below[i][g] * pivots[i], 0.0)
    out = []
    for g in groups:
        size = jnp.sum(jnp.where(lane == row[g], work[g], 0.0), axis=1, keepdims=True)
        valid = (row[g] < count) & (lane >= half) & (lane < half + count)
        out.append(pltpu.roll(jnp.where(valid, work[g] / jnp.sqrt(size), 0.0), half, 1))
    return jnp.concatenate(out, 0)


def krylov_body(raw_ref, out_ref):
    groups, length, width = raw_ref.shape
    out_ref[...] = jnp.zeros(out_ref.shape, F32)
    for j in range(groups):
        out_ref[j * K : j * K + length, :width] = raw_ref[j]
    flat = out_ref[...]
    square = lax.dot_general(
        flat, flat, (((0,), (0,)), ((), ())), precision=HIGHEST, preferred_element_type=F32
    )
    inverse = lower_inverse(square[:K], width)
    inverse = jnp.concatenate([inverse, jnp.zeros((PAD - K, PAD), F32)], 0)
    out_ref[...] = lax.dot_general(flat, inverse, NT, precision=HIGHEST, preferred_element_type=F32)


def sideways(main, side, lane):
    cols = main.shape[-1]
    main_up = pltpu.roll(main, 1, 1)
    side_up = pltpu.roll(side, 1, 1)
    main_down = pltpu.roll(main, cols - 1, 1)
    side_down = pltpu.roll(side, cols - 1, 1)
    first = lane == 0
    last = lane == cols - 1
    left = (jnp.where(first, side_up, main_up), jnp.where(first, main_up, side_up))
    right = (jnp.where(last, side_down, main_down), jnp.where(last, main_down, side_down))
    return left, right


def image_body(
    before_ref, fields_ref, after_ref, left_ref, right_ref,
    tall_ref, side_ref, coef_ref, split_ref, gram_ref,
    local_ref, m1, s1, m2, s2, m3, s3, acc_ref,
):
    total, slots, cols = tall_ref.shape
    rows = total - 2 * HALO
    span = cols // HALO
    lane = lanes((slots, cols))

    def unpack(source, shift, g, carry):
        gathered = [[] for _ in range(8)]
        from_left = left_ref[g]
        from_right = right_ref[g]
        for k in range(span):
            r = g * span + k
            main = source[(g - shift) * span + k]
            tall_ref[r] = main
            turn = (cols - k * HALO) % cols
            low = pltpu.roll(from_right, turn, 1) if turn else from_right
            turn = (cols - HALO - k * HALO) % cols
            high = pltpu.roll(from_left, turn, 1) if turn else from_left
            side = jnp.where(lane < HALO, low, jnp.where(lane >= cols - HALO, high, 0.0))
            packed = []
            for cells in (main, side):
                spin = cells[R + 1 : R + 2]
                couple = COUPLING * cells[R + 2 : R + 3]
                packed += [cells[R : R + 1], spin - couple, -spin - couple, couple]
            local_ref[r] = 2.0 * jnp.concatenate(packed, 0)
            for q in range(8):
                gathered[q].append(packed[q])
            side_ref[r] = side
        for q in range(8):
            coef_ref[q, pl.ds(g * span, span), :] = jnp.concatenate(gathered[q], 0)
        return carry

    first = HALO // span
    last = first + rows // span
    lax.fori_loop(0, first, functools.partial(unpack, before_ref, 0), 0)
    lax.fori_loop(first, last, functools.partial(unpack, fields_ref, first), 0)
    lax.fori_loop(last, last + first, functools.partial(unpack, after_ref, last), 0)

    blank = jnp.zeros((STRIDE - slots, cols), F32)
    size = ORDERS * STRIDE

    def keep(order, r, cells):
        whole = jnp.concatenate([cells, blank], 0)
        high = whole.astype(BF16)
        low = (whole - high.astype(F32)).astype(BF16)
        place = pl.ds(pl.multiple_of((r - HALO) * cols, cols), cols)
        split_ref[order * STRIDE : (order + 1) * STRIDE, place] = high
        split_ref[size + order * STRIDE : size + (order + 1) * STRIDE, place] = low

    def level(order, source, older, target, need_side):
        source_main, source_side = source

        def one(r, store):
            main = source_main[r]
            side = source_side[r]
            local = local_ref[r]
            left, right = sideways(main, side, lane)
            fresh = (
                local[0:1] * main
                + local[1:2] * right[0]
                + local[2:3] * left[0]
                - local[3:4] * (source_main[r - 1] + source_main[r + 1])
            )
            if order == 1:
                fresh = 0.5 * fresh
            if older is not None:
                fresh = fresh - older[0][r]
            if target is not None:
                target[0][r] = fresh
            if need_side:
                edge = (
                    local[4:5] * side
                    + local[5:6] * right[1]
                    + local[6:7] * left[1]
                    - local[7:8] * (source_side[r - 1] + source_side[r + 1])
                )
                if order == 1:
                    edge = 0.5 * edge
                if older is not None:
                    edge = edge - older[1][r]
                target[1][r] = edge
            if store:
                keep(order, r, fresh)

        reach = ORDERS - 1 - order

        def inner(i, carry):
            for k in range(UNROLL):
                one(HALO + i * UNROLL + k, True)
            return carry

        for k in range(reach):
            one(HALO - 1 - k, False)
            one(HALO + rows + k, False)
        lax.fori_loop(0, rows // UNROLL, inner, 0)

    def plain(i, carry):
        for k in range(UNROLL):
            keep(0, HALO + i * UNROLL + k, tall_ref[HALO + i * UNROLL + k])
        return carry

    lax.fori_loop(0, rows // UNROLL, plain, 0)
    level(1, (tall_ref, side_ref), None, (m1, s1), True)
    level(2, (m1, s1), (tall_ref, side_ref), (m2, s2), True)
    level(3, (m2, s2), (m1, s1), (m3, s3), True)
    level(4, (m3, s3), (m2, s2), None, False)

    chunk = rows * cols // 3
    for i in range(3):
        place = slice(i * chunk, (i + 1) * chunk)
        part = lax.dot_general(
            split_ref[:, place], split_ref[:size, place], NT, preferred_element_type=F32
        )
        if i:
            acc_ref[:, :size] += part
        else:
            acc_ref[:, :size] = part
    cross = jnp.concatenate(
        [acc_ref[size:, :size], jnp.zeros((size, WIDE - size), F32)], 1
    )
    cross = jnp.concatenate([cross, jnp.zeros((WIDE - size, WIDE), F32)], 0)
    acc_ref[:size, :size] += (cross + jnp.transpose(cross))[:size, :size]
    lane_wide = lanes((K, WIDE))

    def band(order):
        return acc_ref[order * STRIDE : order * STRIDE + K, :]

    bands = [
        band(0),
        jnp.where(lane_wide < STRIDE, pltpu.roll(band(4), WIDE - 4 * STRIDE, 1), band(1)),
        jnp.where(lane_wide < 2 * STRIDE, pltpu.roll(band(3), WIDE - 3 * STRIDE, 1), band(2)),
    ]
    for i in range(3):
        acc_ref[i * K : (i + 1) * K, :] = bands[i]
    count, _, piece = gram_ref.shape
    deep = piece // WIDE
    for i in range(count):
        for k in range(deep):
            gram_ref[i, :, k * WIDE : (k + 1) * WIDE] = acc_ref[i * deep + k : i * deep + k + 1, :]


def relay_body(parts_ref, spread_ref):
    total = jnp.sum(parts_ref[...], axis=0)
    for i in range(spread_ref.shape[0]):
        spread_ref[i] = total


def absorb(parts, state, turn, inverse_total):
    gram, factor, flipped, square, vectors, pending = state
    new_row = R + turn
    column = KRYLOV + turn
    total = jnp.sum(parts, axis=0) * inverse_total
    table = jnp.concatenate(
        [total[:, a * WIDE : (a + 1) * WIDE] for a in range(ORDERS)]
        + [jnp.zeros((8 - ORDERS, WIDE), F32)],
        0,
    )
    lane_one = lanes((1, WIDE))
    norm = jnp.sum(jnp.where(lane_one == new_row, table[0:1], 0.0), axis=1, keepdims=True)
    beta = jnp.sqrt(norm + EPSILON)
    sigma = 1.0 / beta
    here = (lanes((K, PAD)) == new_row) & (sublanes((K, PAD)) == new_row)
    factor = jnp.where(here, sigma, factor)
    flipped = jnp.where(here, sigma, flipped)
    square = jnp.where(here, sigma * sigma, square)
    tall = jnp.transpose(
        jnp.concatenate([table[:, :PAD], jnp.zeros((PAD - 8, PAD), F32)], 0)
    )
    lane_gram = lanes((K, WIDE))
    gram = jnp.where(sublanes((K, WIDE)) == new_row, table[0:1], gram)
    for b in range(ORDERS):
        gram = jnp.where(lane_gram == b * STRIDE + new_row, tall[:K, b : b + 1], gram)

    latest = [vectors[j * K : (j + 1) * K, column - 1 : column] for j in range(4)]
    unit = (lax.broadcasted_iota(jnp.int32, (K, 1), 0) == new_row).astype(F32)
    expanded = jnp.concatenate(
        [
            latest[1],
            0.5 * (latest[0] + latest[2]),
            0.5 * (latest[1] + latest[3]),
            pending + beta * unit,
        ],
        0,
    )
    first = jnp.sum(vectors * expanded, axis=0, keepdims=True)
    ortho = expanded - jnp.sum(vectors * first, axis=1, keepdims=True)
    second = jnp.sum(vectors * ortho, axis=0, keepdims=True)
    ortho = ortho - jnp.sum(vectors * second, axis=1, keepdims=True)
    eta = jnp.sqrt(jnp.sum(ortho * ortho, axis=0, keepdims=True) + EPSILON)
    vectors = jnp.where(lanes((4 * K, PAD)) == column, ortho / eta, vectors)
    hessenberg = first + second + eta * (lanes((1, PAD)) == column).astype(F32)
    return (gram, factor, flipped, square, vectors, pending), table, sigma, hessenberg


def coefficients_of(state, turn):
    gram, factor, flipped, square, vectors, _ = state
    column = KRYLOV + turn
    latest = [vectors[j * K : (j + 1) * K, column - 1 : column] for j in range(4)]
    mixes = [jnp.sum(factor * one, axis=0, keepdims=True) for one in latest]
    wide = [jnp.concatenate([m, jnp.zeros((1, WIDE - PAD), F32)], 1) for m in mixes]
    target = 0.5 * wide[2]
    for j in range(4):
        target = target - pltpu.roll(0.5 * wide[j], (j + 1) * STRIDE, 1)
    raw = jnp.sum(gram * target, axis=1, keepdims=True)
    upper = jnp.sum(square * raw, axis=0, keepdims=True)
    inside = jnp.where(lanes((K, PAD)) < K, gram[:, :PAD], 0.0)
    twice = 2.0 * raw - jnp.sum(inside * upper, axis=1, keepdims=True)
    removed = jnp.sum(square * twice, axis=0, keepdims=True)
    pending = jnp.sum(
        jnp.where(lanes((K, PAD)) == sublanes((K, PAD)), jnp.sum(flipped * twice, axis=0, keepdims=True), 0.0),
        axis=1,
        keepdims=True,
    )
    table = jnp.concatenate(mixes + [removed] + [jnp.zeros((PAD - 5, PAD), F32)], 0)
    return jnp.transpose(table), mixes + [removed], pending


def turn_body(turn, inverse_total, count, *refs):
    refs = list(refs)
    parts_ref = refs.pop(0)
    state_refs = [refs.pop(0) for _ in range(6 if turn else 1)]
    main_ref, side_ref, coef_ref, split_ref = [refs.pop(0) for _ in range(4)]
    old_fields = [refs.pop(0) for _ in range(turn)]
    old_rows = [refs.pop(0) for _ in range(turn)]
    spread_ref, field_ref, rows_ref, image_ref = [refs.pop(0) for _ in range(4)]
    out_state = [refs.pop(0) for _ in range(6)]
    if turn:
        table_ref, sigma_ref, hessenberg_ref = [refs.pop(0) for _ in range(3)]
    else:
        folded_ref = refs.pop(0)
    z_ref, t_ref, flat_ref = refs

    if turn:
        state = tuple(r[...] for r in state_refs[:5]) + (state_refs[5][:, 0:1],)
        state, table, sigma, hessenberg = absorb(parts_ref[...], state, turn - 1, inverse_total)
        table_ref[...] = table
        sigma_ref[...] = jnp.broadcast_to(sigma, sigma_ref.shape)
        hessenberg_ref[...] = jnp.broadcast_to(hessenberg, hessenberg_ref.shape)
    else:
        pieces, _, piece = parts_ref.shape
        deep = piece // WIDE
        for i in range(pieces):
            for k in range(deep):
                folded_ref[i * deep + k : i * deep + k + 1, :] = (
                    parts_ref[i, :, k * WIDE : (k + 1) * WIDE] * inverse_total
                )
        gram = folded_ref[0:K, :]
        diagonal = lanes((K, PAD)) == sublanes((K, PAD))
        factor = lower_inverse(gram[:, :PAD] + jnp.where(diagonal, GRAM_SHIFT, 0.0), R)
        square = lax.dot_general(
            factor, factor, (((0,), (0,)), ((), ())), precision=HIGHEST, preferred_element_type=F32
        )[:K]
        flipped = jnp.transpose(jnp.concatenate([factor, jnp.zeros((PAD - K, PAD), F32)], 0))[:K]
        state = (gram, factor, flipped, square, state_refs[0][...], None)
    upright, mixes, pending = coefficients_of(state, turn)
    for ref, value in zip(out_state[:5], state[:5]):
        ref[...] = value
    out_state[5][...] = jnp.broadcast_to(pending, out_state[5].shape)

    total, slots, cols = main_ref.shape
    rows = total - 2 * HALO
    raw_only = sublanes((K, cols)) < R
    weights = [jnp.where(raw_only, upright[:K, j : j + 1], 0.0) for j in range(5)]

    def mix_group(g):
        for half, ref in enumerate((main_ref, side_ref)):
            lists = [[] for _ in range(5)]
            for k in range(8):
                cells = ref[g * 8 + k]
                for j in range(5):
                    lists[j].append(jnp.sum(weights[j] * cells, axis=0, keepdims=True))
            for j in range(5):
                z_ref[j, half, pl.ds(pl.multiple_of(g * 8, 8), 8), :] = jnp.concatenate(lists[j], 0)

    def mix(i, carry):
        for k in range(GROUPS):
            mix_group(idle + i * GROUPS + k)
        return carry

    idle = (ORDERS - 1) * turn // 8
    if idle:
        z_ref[:, :, : 8 * idle] = jnp.zeros((5, 2, 8 * idle, cols), F32)
        z_ref[:, :, total - 8 * idle :] = jnp.zeros((5, 2, 8 * idle, cols), F32)
    lax.fori_loop(0, (total // 8 - 2 * idle) // GROUPS, mix, 0)

    z = []
    for j in range(5):
        pair = [z_ref[j, 0], z_ref[j, 1]]
        for s in range(turn):
            scale = mixes[j][:, R + s : R + s + 1]
            pair = [pair[half] + scale * old_fields[s][half] for half in range(2)]
        z.append(pair)

    lane = lanes((total, cols))
    local = [coef_ref[q] for q in range(8)]

    def operate(pair):
        main, side = pair
        left, right = sideways(main, side, lane)
        out = []
        for half, cells in enumerate(pair):
            c = local[4 * half : 4 * half + 4]
            out.append(
                c[0] * cells
                + c[1] * right[half]
                + c[2] * left[half]
                - c[3] * (pltpu.roll(cells, 1, 0) + pltpu.roll(cells, total - 1, 0))
            )
        return out

    def combine(*terms):
        return [sum(w * p[half] for w, p in terms) for half in range(2)]

    four = z[3]
    three = combine((1.0, z[2]), (2.0, operate(four)))
    two = combine((1.0, z[1]), (2.0, operate(three)), (-1.0, four))
    one = combine((1.0, z[0]), (2.0, operate(two)), (-1.0, three))
    summed = combine((1.0, operate(one)), (-1.0, two))
    field = combine((0.5, z[2]), (-0.5, summed), (-1.0, z[4]))
    field_ref[0] = field[0]
    field_ref[1] = field[1]

    images = [field, operate(field)]
    for _ in range(ORDERS - 2):
        images.append(combine((2.0, operate(images[-1])), (-1.0, images[-2])))
    for a in range(ORDERS):
        t_ref[a] = images[a][0]
    image_ref[...] = t_ref[ORDERS - 1, HALO : HALO + rows, :]
    t_ref[ORDERS:] = jnp.zeros((8 - ORDERS, total, cols), F32)
    for r in range(rows):
        flat_ref[:, r * cols : (r + 1) * cols] = t_ref[:, HALO + r, :]

    size = ORDERS * STRIDE
    chunk = rows * cols // 3
    table = jnp.zeros((2 * size, 16), F32)
    own = jnp.zeros((16, 16 * (turn + 1)), F32)
    for i in range(3):
        place = slice(i * chunk, (i + 1) * chunk)
        mine = flat_ref[:, place]
        rounded = mine.astype(BF16).astype(F32)
        both = jnp.concatenate([rounded, mine - rounded], 0).astype(BF16)
        rows_ref[:, place] = both
        table = table + lax.dot_general(
            split_ref[:, place], both, NT, preferred_element_type=F32
        )
        others = jnp.concatenate([ref[:, place] for ref in old_rows] + [both], 0)
        own = own + lax.dot_general(both, others, NT, preferred_element_type=F32)
    own = [
        own[0:8, 16 * s : 16 * s + 8]
        + own[0:8, 16 * s + 8 : 16 * s + 16]
        + own[8:16, 16 * s : 16 * s + 8]
        for s in range(turn + 1)
    ]
    table = table[:size, 0:8] + table[:size, 8:16] + table[size:, 0:8]
    table = jnp.concatenate([table, jnp.zeros((size, PAD - 8), F32)], 1)
    table = jnp.transpose(jnp.concatenate([table, jnp.zeros((WIDE - size, PAD), F32)], 0))[:8]
    lane_table = lanes((8, WIDE))
    for s in range(turn + 1):
        for b in range(ORDERS):
            table = jnp.where(
                lane_table == b * STRIDE + R + s, own[s][:, b : b + 1], table
            )
    flat = jnp.concatenate([table[a : a + 1] for a in range(ORDERS)], 1)
    for i in range(count):
        spread_ref[i] = flat


def final_body(inverse_total, *refs):
    refs = list(refs)
    parts_ref = refs.pop(0)
    state_refs = [refs.pop(0) for _ in range(6)]
    folded_ref = refs.pop(0)
    old_tables = [refs.pop(0) for _ in range(STEPS - 1)]
    old_sigmas = [refs.pop(0) for _ in range(STEPS - 1)]
    old_hessen = [refs.pop(0) for _ in range(STEPS - 1)]
    fields = [refs.pop(0) for _ in range(STEPS)]
    images = [refs.pop(0) for _ in range(STEPS)]
    columns_ref, coefficients_ref, hessenberg_ref, gram_ref, image_ref = refs

    state = tuple(r[...] for r in state_refs[:5]) + (state_refs[5][:, 0:1],)
    state, table, sigma, hessenberg = absorb(parts_ref[...], state, STEPS - 1, inverse_total)
    factor = state[1]
    flat = jnp.concatenate([state[4], jnp.zeros((WIDE - 4 * K, PAD), F32)], 0)
    flat = jnp.transpose(flat)[:WIDTH]
    for j in range(4):
        coefficients_ref[:, j, :] = flat[:, j * K : (j + 1) * K]
    hessenberg_ref[...] = jnp.concatenate([r[0:1] for r in old_hessen] + [hessenberg], 0)[:, :WIDTH]
    sigmas = [ref[0:1, 0:1] for ref in old_sigmas] + [sigma]
    rows = columns_ref.shape[1]
    for s in range(STEPS):
        columns_ref[s] = sigmas[s] * fields[s][0, HALO : HALO + rows, :]
        image_ref[s] = sigmas[s] * images[s][...]

    lane_wide = lanes((K, WIDE))
    bands = [folded_ref[i * K : (i + 1) * K, :] for i in range(3)]
    upper = [
        bands[0],
        bands[1],
        bands[2],
        pltpu.roll(bands[2], 3 * STRIDE, 1),
        pltpu.roll(bands[1], 4 * STRIDE, 1),
    ]
    blank = jnp.zeros((STRIDE - K, WIDE), F32)
    stacked = []
    for a in range(ORDERS):
        stacked += [jnp.where((lane_wide >= a * STRIDE) & (lane_wide < ORDERS * STRIDE), upper[a], 0.0), blank]
    whole = jnp.concatenate(stacked + [jnp.zeros((WIDE - ORDERS * STRIDE, WIDE), F32)], 0)
    row_id = sublanes((WIDE, WIDE))
    lane_id = lanes((WIDE, WIDE))
    lower = row_id >= (lane_id // STRIDE + 1) * STRIDE
    whole = jnp.where(lower, jnp.transpose(whole), whole)
    for s, one in enumerate([ref[...] for ref in old_tables] + [table]):
        flipped = jnp.transpose(jnp.concatenate([one, jnp.zeros((PAD - 8, WIDE), F32)], 0))
        for a in range(ORDERS):
            whole = jnp.where(row_id == a * STRIDE + R + s, one[a : a + 1, :], whole)
        for a in range(ORDERS):
            whole = jnp.where(lane_id == a * STRIDE + R + s, flipped[:, a : a + 1], whole)
    padded = jnp.concatenate([factor, jnp.zeros((K, WIDE - PAD), F32)], 1)
    padded = jnp.concatenate([padded, blank], 0)
    blocks = [padded] + [pltpu.roll(padded, a * STRIDE, 1) for a in range(1, ORDERS)]
    diagonal = jnp.concatenate(blocks + [jnp.zeros((WIDE - ORDERS * STRIDE, WIDE), F32)], 0)
    half = jnp.dot(diagonal, whole, precision=HIGHEST, preferred_element_type=F32)
    done = lax.dot_general(half, diagonal, NT, precision=HIGHEST, preferred_element_type=F32)
    for a in range(ORDERS):
        for b in range(ORDERS):
            gram_ref[a, b] = done[a * STRIDE : a * STRIDE + K, b * STRIDE : b * STRIDE + K]


def shape(*dims, dtype=F32):
    return jax.ShapeDtypeStruct(dims, dtype)


def local(basis_raw, krylov_raw, stiffness, rotation):
    rows = basis_raw.shape[1]
    cols = basis_raw.shape[2]
    cells = rows * cols
    count = device_count()
    inverse_total = 1.0 / (cells * count)
    total = rows + 2 * HALO
    size = ORDERS * STRIDE

    fields = jnp.concatenate(
        [
            jnp.transpose(basis_raw, (1, 0, 2)),
            stiffness[:, None],
            rotation[:, None],
            jnp.ones((rows, 1, cols), F32),
        ],
        1,
    )
    up, down = shifts("row")
    before = lax.ppermute(fields[rows - HALO :], "row", up)
    after = lax.ppermute(fields[:HALO], "row", down)
    pieces = (before, fields, after)
    strip = shape(total * HALO // cols, K, cols)
    low, high = pl.pallas_call(pack_body, out_shape=(strip, strip), name="pack", compiler_params=SMALL)(*pieces)
    up, down = shifts("col")
    from_left = lax.ppermute(high, "col", up)
    from_right = lax.ppermute(low, "col", down)
    vectors = pl.pallas_call(krylov_body, out_shape=shape(4 * K, PAD), name="krylov", compiler_params=SMALL)(krylov_raw)
    vectors, from_left = lax.optimization_barrier((vectors, from_left))

    level = pltpu.VMEM((total, K, cols), F32)
    piece = PAD * WIDE // count
    tall, side, coefs, split, folded = pl.pallas_call(
        image_body,
        out_shape=(
            shape(total, K, cols),
            shape(total, K, cols),
            shape(8, total, cols),
            shape(2 * size, cells, dtype=BF16),
            shape(count, 1, piece),
        ),
        scratch_shapes=[pltpu.VMEM((total, 8, cols), F32)]
        + [level] * 6
        + [pltpu.VMEM((2 * size, WIDE), F32)],
        name="images", compiler_params=LARGE,
    )(*pieces, from_left, from_right)

    mine = pl.pallas_call(
        relay_body, out_shape=shape(count, 1, piece), name="relay", compiler_params=SMALL
    )(exchange(folded))
    parts = exchange(mine)

    state_shapes = (
        shape(K, WIDE),
        shape(K, PAD),
        shape(K, PAD),
        shape(K, PAD),
        shape(4 * K, PAD),
        shape(K, PAD),
    )
    state = (vectors,)
    made_fields, made_rows, made_images, tables, sigmas, hessen = [], [], [], [], [], []
    for turn in range(STEPS):
        out_shape = (
            shape(count, 1, ORDERS * WIDE),
            shape(2, total, cols),
            shape(16, cells, dtype=BF16),
            shape(rows, cols),
        ) + state_shapes
        if turn:
            out_shape += (shape(8, WIDE), shape(8, PAD), shape(8, PAD))
        else:
            out_shape += (shape(PAD, WIDE),)
        outs = pl.pallas_call(
            functools.partial(turn_body, turn, inverse_total, count),
            out_shape=out_shape,
            scratch_shapes=[
                pltpu.VMEM((5, 2, total, cols), F32),
                pltpu.VMEM((8, total, cols), F32),
                pltpu.VMEM((8, cells), F32),
            ],
            name=f"turn{turn}", compiler_params=LARGE,
        )(parts, *state, tall, side, coefs, split, *made_fields, *made_rows)
        made_fields.append(outs[1])
        made_rows.append(outs[2])
        made_images.append(outs[3])
        state = outs[4:10]
        if turn:
            tables.append(outs[10])
            sigmas.append(outs[11])
            hessen.append(outs[12])
        else:
            folded = outs[10]
        parts = exchange(outs[0])

    new_columns, coefficients, hessenberg, gram, new_images = pl.pallas_call(
        functools.partial(final_body, inverse_total),
        out_shape=(
            shape(STEPS, rows, cols),
            shape(WIDTH, 4, K),
            shape(STEPS, WIDTH),
            shape(ORDERS, ORDERS, K, K),
            shape(STEPS, rows, cols),
        ),
        name="final", compiler_params=SMALL,
    )(parts, *state, folded, *tables, *sigmas, *hessen, *made_fields, *made_images)
    gram = jnp.transpose(gram, (0, 2, 1, 3))
    coefficients = jnp.transpose(coefficients, (1, 2, 0))
    return (new_columns, coefficients, hessenberg, gram, new_images)


def solution(mesh):
    in_specs = (P(None, "row", "col"), P(), P("row", "col"), P("row", "col"))
    out_specs = (P(None, "row", "col"), P(), P(), P(), P(None, "row", "col"))
    return jax.shard_map(local, mesh=mesh, in_specs=in_specs, out_specs=out_specs, check_vma=False)
```

```python
import functools
import jax
import jax.numpy as jnp
from jax import lax
from jax.experimental import pallas as pl
from jax.experimental.pallas import tpu as pltpu
from jax.sharding import PartitionSpec as P

K = 40
STEPS = 3
R = 37
KRYLOV = 34
WIDTH = KRYLOV + STEPS

COUPLING = 0.2
EPSILON = 1e-06
GRAM_SHIFT = 0.05
HIGHEST = lax.Precision.HIGHEST
F32 = jnp.float32
BF16 = jnp.bfloat16

ORDERS = 5
HALO = (ORDERS - 1) * (STEPS + 1)
STRIDE = 48
WIDE = 256
SMALL = pltpu.CompilerParams(vmem_limit_bytes=8 << 20)
LARGE = pltpu.CompilerParams(vmem_limit_bytes=24 << 20)
PAD = 128
AXES = ("row", "col")
NT = (((1,), (1,)), ((), ()))


def device_count():
    return lax.axis_size("row") * lax.axis_size("col")


def exchange(spread):
    return lax.all_to_all(spread, AXES, 0, 0, tiled=True)


def shifts(axis):
    peers = lax.axis_size(axis)
    up = [(i, i + 1) for i in range(peers - 1)]
    return up, [(j, i) for i, j in up]


def lanes(shape):
    return lax.broadcasted_iota(jnp.int32, shape, len(shape) - 1)


def sublanes(shape):
    return lax.broadcasted_iota(jnp.int32, shape, len(shape) - 2)


def pack_body(before_ref, fields_ref, after_ref, low_ref, high_ref):
    rows, slots, cols = fields_ref.shape
    span = cols // HALO
    lane = lanes((slots, cols))
    edge = HALO // span

    def group(source, shift, g, carry):
        low = jnp.zeros((slots, cols), F32)
        high = jnp.zeros((slots, cols), F32)
        for k in range(span):
            cells = source[(g - shift) * span + k]
            inside = (lane >= k * HALO) & (lane < (k + 1) * HALO)
            first = pltpu.roll(cells, k * HALO, 1) if k else cells
            turn = (k * HALO + HALO) % cols
            second = pltpu.roll(cells, turn, 1) if turn else cells
            low = jnp.where(inside, first, low)
            high = jnp.where(inside, second, high)
        low_ref[g] = low
        high_ref[g] = high
        return carry

    last = edge + rows // span
    for g in range(0, edge):
        group(before_ref, 0, g, 0)
    for g in range(edge, last):
        group(fields_ref, edge, g, 0)
    for g in range(last, last + edge):
        group(after_ref, last, g, 0)


def lower_inverse(matrix, count):
    half = PAD // 2
    block = 4
    tile = (8, PAD)
    groups = range(K // 8)
    lane = lanes(tile)
    row = [sublanes(tile) + 8 * g for g in groups]
    work = []
    for g in groups:
        used = (row[g] < count) & (lane < count)
        left = jnp.where(used, matrix[8 * g : 8 * g + 8], (lane == row[g]).astype(F32))
        work.append(jnp.where(lane < half, left, (lane == row[g] + half).astype(F32)))
    for start in range(0, K, block):
        active = [g for g in groups if 8 * g + 7 > start]
        spots = range(start, start + block)
        pivots = [jnp.broadcast_to(work[j // 8][j % 8 : j % 8 + 1], tile) for j in spots]
        below = [
            {g: jnp.broadcast_to(work[g][:, j : j + 1], tile) for g in active} for j in spots
        ]
        corner = [
            [jnp.broadcast_to(pivots[i][:, j : j + 1], tile) for j in spots] for i in range(block)
        ]
        for i in range(block):
            inverse = 1.0 / corner[i][i]
            for k in range(i + 1, block):
                ratio = corner[i][k] * inverse
                pivots[k] = pivots[k] - pivots[i] * ratio
                for g in active:
                    below[k][g] = below[k][g] - below[i][g] * ratio
                for other in range(k, block):
                    corner[k][other] = corner[k][other] - corner[i][other] * ratio
            below[i] = {g: below[i][g] * inverse for g in active}
        for g in active:
            for i in range(block):
                work[g] = work[g] - jnp.where(row[g] > start + i, below[i][g] * pivots[i], 0.0)
    out = []
    for g in groups:
        size = jnp.sum(jnp.where(lane == row[g], work[g], 0.0), axis=1, keepdims=True)
        valid = (row[g] < count) & (lane >= half) & (lane < half + count)
        out.append(pltpu.roll(jnp.where(valid, work[g] / jnp.sqrt(size), 0.0), half, 1))
    return jnp.concatenate(out, 0)


def krylov_body(raw_ref, out_ref):
    groups, length, width = raw_ref.shape
    out_ref[...] = jnp.zeros(out_ref.shape, F32)
    for j in range(groups):
        out_ref[j * K : j * K + length, :width] = raw_ref[j]
    flat = out_ref[...]
    square = lax.dot_general(
        flat, flat, (((0,), (0,)), ((), ())), precision=HIGHEST, preferred_element_type=F32
    )
    inverse = lower_inverse(square[:K], width)
    inverse = jnp.concatenate([inverse, jnp.zeros((PAD - K, PAD), F32)], 0)
    out_ref[...] = lax.dot_general(flat, inverse, NT, precision=HIGHEST, preferred_element_type=F32)


def sideways(main, side, lane):
    cols = main.shape[-1]
    main_up = pltpu.roll(main, 1, 1)
    side_up = pltpu.roll(side, 1, 1)
    main_down = pltpu.roll(main, cols - 1, 1)
    side_down = pltpu.roll(side, cols - 1, 1)
    first = lane == 0
    last = lane == cols - 1
    left = (jnp.where(first, side_up, main_up), jnp.where(first, main_up, side_up))
    right = (jnp.where(last, side_down, main_down), jnp.where(last, main_down, side_down))
    return left, right


def image_body(
    before_ref, fields_ref, after_ref, left_ref, right_ref,
    tall_ref, side_ref, coef_ref, split_ref, gram_ref,
    local_ref, m1, s1, m2, s2, m3, s3, acc_ref,
):
    total, slots, cols = tall_ref.shape
    rows = total - 2 * HALO
    span = cols // HALO
    lane = lanes((slots, cols))

    def unpack(source, shift, g, carry):
        gathered = [[] for _ in range(8)]
        from_left = left_ref[g]
        from_right = right_ref[g]
        for k in range(span):
            r = g * span + k
            main = source[(g - shift) * span + k]
            tall_ref[r] = main
            turn = (cols - k * HALO) % cols
            low = pltpu.roll(from_right, turn, 1) if turn else from_right
            turn = (cols - HALO - k * HALO) % cols
            high = pltpu.roll(from_left, turn, 1) if turn else from_left
            side = jnp.where(lane < HALO, low, jnp.where(lane >= cols - HALO, high, 0.0))
            packed = []
            for cells in (main, side):
                spin = cells[R + 1 : R + 2]
                couple = COUPLING * cells[R + 2 : R + 3]
                packed += [cells[R : R + 1], spin - couple, -spin - couple, couple]
            local_ref[r] = 2.0 * jnp.concatenate(packed, 0)
            for q in range(8):
                gathered[q].append(packed[q])
            side_ref[r] = side
        for q in range(8):
            coef_ref[q, pl.ds(g * span, span), :] = jnp.concatenate(gathered[q], 0)
        return carry

    first = HALO // span
    last = first + rows // span
    for g in range(0, first):
        unpack(before_ref, 0, g, 0)
    for g in range(first, last):
        unpack(fields_ref, first, g, 0)
    for g in range(last, last + first):
        unpack(after_ref, last, g, 0)

    blank = jnp.zeros((STRIDE - slots, cols), F32)
    size = ORDERS * STRIDE

    def keep(order, r, cells):
        whole = jnp.concatenate([cells, blank], 0)
        high = whole.astype(BF16)
        low = (whole - high.astype(F32)).astype(BF16)
        place = slice((r - HALO) * cols, (r - HALO + 1) * cols)
        split_ref[order * STRIDE : (order + 1) * STRIDE, place] = high
        split_ref[size + order * STRIDE : size + (order + 1) * STRIDE, place] = low

    def level(order, source, older, target, need_side):
        source_main, source_side = source

        def one(r, store):
            main = source_main[r]
            side = source_side[r]
            local = local_ref[r]
            left, right = sideways(main, side, lane)
            fresh = (
                local[0:1] * main
                + local[1:2] * right[0]
                + local[2:3] * left[0]
                - local[3:4] * (source_main[r - 1] + source_main[r + 1])
            )
            if order == 1:
                fresh = 0.5 * fresh
            if older is not None:
                fresh = fresh - older[0][r]
            if target is not None:
                target[0][r] = fresh
            if need_side:
                edge = (
                    local[4:5] * side
                    + local[5:6] * right[1]
                    + local[6:7] * left[1]
                    - local[7:8] * (source_side[r - 1] + source_side[r + 1])
                )
                if order == 1:
                    edge = 0.5 * edge
                if older is not None:
                    edge = edge - older[1][r]
                target[1][r] = edge
            if store:
                keep(order, r, fresh)

        reach = ORDERS - 1 - order

        for k in range(reach):
            one(HALO - 1 - k, False)
            one(HALO + rows + k, False)
        for r in range(HALO, HALO + rows):
            one(r, True)

    for r in range(HALO, HALO + rows):
        keep(0, r, tall_ref[r])
    level(1, (tall_ref, side_ref), None, (m1, s1), True)
    level(2, (m1, s1), (tall_ref, side_ref), (m2, s2), True)
    level(3, (m2, s2), (m1, s1), (m3, s3), True)
    level(4, (m3, s3), (m2, s2), None, False)

    chunk = rows * cols // 3
    for i in range(3):
        place = slice(i * chunk, (i + 1) * chunk)
        part = lax.dot_general(
            split_ref[:, place], split_ref[:size, place], NT, preferred_element_type=F32
        )
        if i:
            acc_ref[:, :size] += part
        else:
            acc_ref[:, :size] = part
    cross = jnp.concatenate(
        [acc_ref[size:, :size], jnp.zeros((size, WIDE - size), F32)], 1
    )
    cross = jnp.concatenate([cross, jnp.zeros((WIDE - size, WIDE), F32)], 0)
    acc_ref[:size, :size] += (cross + jnp.transpose(cross))[:size, :size]
    lane_wide = lanes((K, WIDE))

    def band(order):
        return acc_ref[order * STRIDE : order * STRIDE + K, :]

    bands = [
        band(0),
        jnp.where(lane_wide < STRIDE, pltpu.roll(band(4), WIDE - 4 * STRIDE, 1), band(1)),
        jnp.where(lane_wide < 2 * STRIDE, pltpu.roll(band(3), WIDE - 3 * STRIDE, 1), band(2)),
    ]
    for i in range(3):
        acc_ref[i * K : (i + 1) * K, :] = bands[i]
    count, _, piece = gram_ref.shape
    width = min(piece, WIDE)
    for i in range(count):
        for k in range(0, piece, width):
            spot, start = divmod(i * piece + k, WIDE)
            gram_ref[i, :, k : k + width] = acc_ref[spot : spot + 1, start : start + width]


def relay_body(parts_ref, spread_ref):
    total = jnp.sum(parts_ref[...], axis=0)
    for i in range(spread_ref.shape[0]):
        spread_ref[i] = total


def absorb(parts, state, turn, inverse_total):
    gram, factor, flipped, square, vectors, pending = state
    new_row = R + turn
    column = KRYLOV + turn
    total = jnp.sum(parts, axis=0) * inverse_total
    table = jnp.concatenate(
        [total[:, a * WIDE : (a + 1) * WIDE] for a in range(ORDERS)]
        + [jnp.zeros((8 - ORDERS, WIDE), F32)],
        0,
    )
    lane_one = lanes((1, WIDE))
    norm = jnp.sum(jnp.where(lane_one == new_row, table[0:1], 0.0), axis=1, keepdims=True)
    beta = jnp.sqrt(norm + EPSILON)
    sigma = 1.0 / beta
    here = (lanes((K, PAD)) == new_row) & (sublanes((K, PAD)) == new_row)
    factor = jnp.where(here, sigma, factor)
    flipped = jnp.where(here, sigma, flipped)
    square = jnp.where(here, sigma * sigma, square)
    tall = jnp.transpose(
        jnp.concatenate([table[:, :PAD], jnp.zeros((PAD - 8, PAD), F32)], 0)
    )
    lane_gram = lanes((K, WIDE))
    gram = jnp.where(sublanes((K, WIDE)) == new_row, table[0:1], gram)
    for b in range(ORDERS):
        gram = jnp.where(lane_gram == b * STRIDE + new_row, tall[:K, b : b + 1], gram)

    latest = [vectors[j * K : (j + 1) * K, column - 1 : column] for j in range(4)]
    unit = (lax.broadcasted_iota(jnp.int32, (K, 1), 0) == new_row).astype(F32)
    expanded = jnp.concatenate(
        [
            latest[1],
            0.5 * (latest[0] + latest[2]),
            0.5 * (latest[1] + latest[3]),
            pending + beta * unit,
        ],
        0,
    )
    first = jnp.sum(vectors * expanded, axis=0, keepdims=True)
    ortho = expanded - jnp.sum(vectors * first, axis=1, keepdims=True)
    second = jnp.sum(vectors * ortho, axis=0, keepdims=True)
    ortho = ortho - jnp.sum(vectors * second, axis=1, keepdims=True)
    eta = jnp.sqrt(jnp.sum(ortho * ortho, axis=0, keepdims=True) + EPSILON)
    vectors = jnp.where(lanes((4 * K, PAD)) == column, ortho / eta, vectors)
    hessenberg = first + second + eta * (lanes((1, PAD)) == column).astype(F32)
    return (gram, factor, flipped, square, vectors, pending), table, sigma, hessenberg


def coefficients_of(state, turn):
    gram, factor, flipped, square, vectors, _ = state
    column = KRYLOV + turn
    latest = [vectors[j * K : (j + 1) * K, column - 1 : column] for j in range(4)]
    mixes = [jnp.sum(factor * one, axis=0, keepdims=True) for one in latest]
    wide = [jnp.concatenate([m, jnp.zeros((1, WIDE - PAD), F32)], 1) for m in mixes]
    target = 0.5 * wide[2]
    for j in range(4):
        target = target - pltpu.roll(0.5 * wide[j], (j + 1) * STRIDE, 1)
    raw = jnp.sum(gram * target, axis=1, keepdims=True)
    upper = jnp.sum(square * raw, axis=0, keepdims=True)
    inside = jnp.where(lanes((K, PAD)) < K, gram[:, :PAD], 0.0)
    twice = 2.0 * raw - jnp.sum(inside * upper, axis=1, keepdims=True)
    removed = jnp.sum(square * twice, axis=0, keepdims=True)
    pending = jnp.sum(
        jnp.where(lanes((K, PAD)) == sublanes((K, PAD)), jnp.sum(flipped * twice, axis=0, keepdims=True), 0.0),
        axis=1,
        keepdims=True,
    )
    table = jnp.concatenate(mixes + [removed] + [jnp.zeros((PAD - 5, PAD), F32)], 0)
    return jnp.transpose(table), mixes + [removed], pending


def turn_body(turn, inverse_total, count, *refs):
    refs = list(refs)
    parts_ref = refs.pop(0)
    state_refs = [refs.pop(0) for _ in range(6 if turn else 1)]
    main_ref, side_ref, coef_ref, split_ref = [refs.pop(0) for _ in range(4)]
    old_fields = [refs.pop(0) for _ in range(turn)]
    old_rows = [refs.pop(0) for _ in range(turn)]
    spread_ref, field_ref, rows_ref, image_ref = [refs.pop(0) for _ in range(4)]
    out_state = [refs.pop(0) for _ in range(6)]
    if turn:
        table_ref, sigma_ref, hessenberg_ref = [refs.pop(0) for _ in range(3)]
    else:
        folded_ref = refs.pop(0)
    z_ref, t_ref, flat_ref = refs

    if turn:
        state = tuple(r[...] for r in state_refs[:5]) + (state_refs[5][:, 0:1],)
        state, table, sigma, hessenberg = absorb(parts_ref[...], state, turn - 1, inverse_total)
        table_ref[...] = table
        sigma_ref[...] = jnp.broadcast_to(sigma, sigma_ref.shape)
        hessenberg_ref[...] = jnp.broadcast_to(hessenberg, hessenberg_ref.shape)
    else:
        pieces, _, piece = parts_ref.shape
        width = min(piece, WIDE)
        for i in range(pieces):
            for k in range(0, piece, width):
                spot, start = divmod(i * piece + k, WIDE)
                folded_ref[spot : spot + 1, start : start + width] = (
                    parts_ref[i, :, k : k + width] * inverse_total
                )
        gram = folded_ref[0:K, :]
        diagonal = lanes((K, PAD)) == sublanes((K, PAD))
        factor = lower_inverse(gram[:, :PAD] + jnp.where(diagonal, GRAM_SHIFT, 0.0), R)
        square = lax.dot_general(
            factor, factor, (((0,), (0,)), ((), ())), precision=HIGHEST, preferred_element_type=F32
        )[:K]
        flipped = jnp.transpose(jnp.concatenate([factor, jnp.zeros((PAD - K, PAD), F32)], 0))[:K]
        state = (gram, factor, flipped, square, state_refs[0][...], None)
    upright, mixes, pending = coefficients_of(state, turn)
    for ref, value in zip(out_state[:5], state[:5]):
        ref[...] = value
    out_state[5][...] = jnp.broadcast_to(pending, out_state[5].shape)

    total, slots, cols = main_ref.shape
    rows = total - 2 * HALO
    raw_only = sublanes((K, cols)) < R
    weights = [jnp.where(raw_only, upright[:K, j : j + 1], 0.0) for j in range(5)]

    def mix_group(g):
        for half, ref in enumerate((main_ref, side_ref)):
            lists = [[] for _ in range(5)]
            for k in range(8):
                cells = ref[g * 8 + k]
                for j in range(5):
                    lists[j].append(jnp.sum(weights[j] * cells, axis=0, keepdims=True))
            for j in range(5):
                z_ref[j, half, pl.ds(pl.multiple_of(g * 8, 8), 8), :] = jnp.concatenate(lists[j], 0)

    def mix(i, carry):
        for k in range(groups):
            mix_group(idle + i * groups + k)
        return carry

    idle = (ORDERS - 1) * turn // 8
    groups = (total // 8 - 2 * idle) // 2
    if idle:
        z_ref[:, :, : 8 * idle] = jnp.zeros((5, 2, 8 * idle, cols), F32)
        z_ref[:, :, total - 8 * idle :] = jnp.zeros((5, 2, 8 * idle, cols), F32)
    lax.fori_loop(0, 2, mix, 0)

    z = []
    for j in range(5):
        pair = [z_ref[j, 0], z_ref[j, 1]]
        for s in range(turn):
            scale = mixes[j][:, R + s : R + s + 1]
            pair = [pair[half] + scale * old_fields[s][half] for half in range(2)]
        z.append(pair)

    lane = lanes((total, cols))
    local = [coef_ref[q] for q in range(8)]

    def operate(pair):
        main, side = pair
        left, right = sideways(main, side, lane)
        out = []
        for half, cells in enumerate(pair):
            c = local[4 * half : 4 * half + 4]
            out.append(
                c[0] * cells
                + c[1] * right[half]
                + c[2] * left[half]
                - c[3] * (pltpu.roll(cells, 1, 0) + pltpu.roll(cells, total - 1, 0))
            )
        return out

    def combine(*terms):
        return [sum(w * p[half] for w, p in terms) for half in range(2)]

    four = z[3]
    three = combine((1.0, z[2]), (2.0, operate(four)))
    two = combine((1.0, z[1]), (2.0, operate(three)), (-1.0, four))
    one = combine((1.0, z[0]), (2.0, operate(two)), (-1.0, three))
    summed = combine((1.0, operate(one)), (-1.0, two))
    field = combine((0.5, z[2]), (-0.5, summed), (-1.0, z[4]))
    field_ref[0] = field[0]
    field_ref[1] = field[1]

    images = [field, operate(field)]
    for _ in range(ORDERS - 2):
        images.append(combine((2.0, operate(images[-1])), (-1.0, images[-2])))
    for a in range(ORDERS):
        t_ref[a] = images[a][0]
    image_ref[...] = t_ref[ORDERS - 1, HALO : HALO + rows, :]
    t_ref[ORDERS:] = jnp.zeros((8 - ORDERS, total, cols), F32)
    for r in range(rows):
        flat_ref[:, r * cols : (r + 1) * cols] = t_ref[:, HALO + r, :]

    size = ORDERS * STRIDE
    chunk = rows * cols // 3
    table = jnp.zeros((2 * size, 16), F32)
    own = jnp.zeros((16, 16 * (turn + 1)), F32)
    for i in range(3):
        place = slice(i * chunk, (i + 1) * chunk)
        mine = flat_ref[:, place]
        rounded = mine.astype(BF16).astype(F32)
        both = jnp.concatenate([rounded, mine - rounded], 0).astype(BF16)
        rows_ref[:, place] = both
        table = table + lax.dot_general(
            split_ref[:, place], both, NT, preferred_element_type=F32
        )
        others = jnp.concatenate([ref[:, place] for ref in old_rows] + [both], 0)
        own = own + lax.dot_general(both, others, NT, preferred_element_type=F32)
    own = [
        own[0:8, 16 * s : 16 * s + 8]
        + own[0:8, 16 * s + 8 : 16 * s + 16]
        + own[8:16, 16 * s : 16 * s + 8]
        for s in range(turn + 1)
    ]
    table = table[:size, 0:8] + table[:size, 8:16] + table[size:, 0:8]
    table = jnp.concatenate([table, jnp.zeros((size, PAD - 8), F32)], 1)
    table = jnp.transpose(jnp.concatenate([table, jnp.zeros((WIDE - size, PAD), F32)], 0))[:8]
    lane_table = lanes((8, WIDE))
    for s in range(turn + 1):
        for b in range(ORDERS):
            table = jnp.where(
                lane_table == b * STRIDE + R + s, own[s][:, b : b + 1], table
            )
    flat = jnp.concatenate([table[a : a + 1] for a in range(ORDERS)], 1)
    for i in range(count):
        spread_ref[i] = flat


def final_body(inverse_total, *refs):
    refs = list(refs)
    parts_ref = refs.pop(0)
    state_refs = [refs.pop(0) for _ in range(6)]
    folded_ref = refs.pop(0)
    old_tables = [refs.pop(0) for _ in range(STEPS - 1)]
    old_sigmas = [refs.pop(0) for _ in range(STEPS - 1)]
    old_hessen = [refs.pop(0) for _ in range(STEPS - 1)]
    fields = [refs.pop(0) for _ in range(STEPS)]
    images = [refs.pop(0) for _ in range(STEPS)]
    columns_ref, coefficients_ref, hessenberg_ref, gram_ref, image_ref = refs

    state = tuple(r[...] for r in state_refs[:5]) + (state_refs[5][:, 0:1],)
    state, table, sigma, hessenberg = absorb(parts_ref[...], state, STEPS - 1, inverse_total)
    factor = state[1]
    flat = jnp.concatenate([state[4], jnp.zeros((WIDE - 4 * K, PAD), F32)], 0)
    flat = jnp.transpose(flat)[:WIDTH]
    for j in range(4):
        coefficients_ref[:, j, :] = flat[:, j * K : (j + 1) * K]
    hessenberg_ref[...] = jnp.concatenate([r[0:1] for r in old_hessen] + [hessenberg], 0)[:, :WIDTH]
    sigmas = [ref[0:1, 0:1] for ref in old_sigmas] + [sigma]
    rows = columns_ref.shape[1]
    for s in range(STEPS):
        columns_ref[s] = sigmas[s] * fields[s][0, HALO : HALO + rows, :]
        image_ref[s] = sigmas[s] * images[s][...]

    lane_wide = lanes((K, WIDE))
    bands = [folded_ref[i * K : (i + 1) * K, :] for i in range(3)]
    upper = [
        bands[0],
        bands[1],
        bands[2],
        pltpu.roll(bands[2], 3 * STRIDE, 1),
        pltpu.roll(bands[1], 4 * STRIDE, 1),
    ]
    blank = jnp.zeros((STRIDE - K, WIDE), F32)
    stacked = []
    for a in range(ORDERS):
        stacked += [jnp.where((lane_wide >= a * STRIDE) & (lane_wide < ORDERS * STRIDE), upper[a], 0.0), blank]
    whole = jnp.concatenate(stacked + [jnp.zeros((WIDE - ORDERS * STRIDE, WIDE), F32)], 0)
    row_id = sublanes((WIDE, WIDE))
    lane_id = lanes((WIDE, WIDE))
    lower = row_id >= (lane_id // STRIDE + 1) * STRIDE
    whole = jnp.where(lower, jnp.transpose(whole), whole)
    for s, one in enumerate([ref[...] for ref in old_tables] + [table]):
        flipped = jnp.transpose(jnp.concatenate([one, jnp.zeros((PAD - 8, WIDE), F32)], 0))
        for a in range(ORDERS):
            whole = jnp.where(row_id == a * STRIDE + R + s, one[a : a + 1, :], whole)
        for a in range(ORDERS):
            whole = jnp.where(lane_id == a * STRIDE + R + s, flipped[:, a : a + 1], whole)
    padded = jnp.concatenate([factor, jnp.zeros((K, WIDE - PAD), F32)], 1)
    padded = jnp.concatenate([padded, blank], 0)
    blocks = [padded] + [pltpu.roll(padded, a * STRIDE, 1) for a in range(1, ORDERS)]
    diagonal = jnp.concatenate(blocks + [jnp.zeros((WIDE - ORDERS * STRIDE, WIDE), F32)], 0)
    half = jnp.dot(diagonal, whole, precision=HIGHEST, preferred_element_type=F32)
    done = lax.dot_general(half, diagonal, NT, precision=HIGHEST, preferred_element_type=F32)
    for a in range(ORDERS):
        for b in range(ORDERS):
            gram_ref[a, b] = done[a * STRIDE : a * STRIDE + K, b * STRIDE : b * STRIDE + K]


def shape(*dims, dtype=F32):
    return jax.ShapeDtypeStruct(dims, dtype)


def local(basis_raw, krylov_raw, stiffness, rotation):
    rows = basis_raw.shape[1]
    cols = basis_raw.shape[2]
    cells = rows * cols
    count = device_count()
    inverse_total = 1.0 / (cells * count)
    total = rows + 2 * HALO
    size = ORDERS * STRIDE

    fields = jnp.concatenate(
        [
            jnp.transpose(basis_raw, (1, 0, 2)),
            stiffness[:, None],
            rotation[:, None],
            jnp.ones((rows, 1, cols), F32),
        ],
        1,
    )
    up, down = shifts("row")
    before = lax.ppermute(fields[rows - HALO :], "row", up)
    after = lax.ppermute(fields[:HALO], "row", down)
    pieces = (before, fields, after)
    strip = shape(total * HALO // cols, K, cols)
    low, high = pl.pallas_call(pack_body, out_shape=(strip, strip), name="pack", compiler_params=SMALL)(*pieces)
    up, down = shifts("col")
    from_left = lax.ppermute(high, "col", up)
    from_right = lax.ppermute(low, "col", down)
    vectors = pl.pallas_call(krylov_body, out_shape=shape(4 * K, PAD), name="krylov", compiler_params=SMALL)(krylov_raw)
    vectors, from_left = lax.optimization_barrier((vectors, from_left))

    level = pltpu.VMEM((total, K, cols), F32)
    piece = PAD * WIDE // count
    tall, side, coefs, split, folded = pl.pallas_call(
        image_body,
        out_shape=(
            shape(total, K, cols),
            shape(total, K, cols),
            shape(8, total, cols),
            shape(2 * size, cells, dtype=BF16),
            shape(count, 1, piece),
        ),
        scratch_shapes=[pltpu.VMEM((total, 8, cols), F32)]
        + [level] * 6
        + [pltpu.VMEM((2 * size, WIDE), F32)],
        name="images", compiler_params=LARGE,
    )(*pieces, from_left, from_right)

    mine = pl.pallas_call(
        relay_body, out_shape=shape(count, 1, piece), name="relay", compiler_params=SMALL
    )(exchange(folded))
    parts = exchange(mine)

    state_shapes = (
        shape(K, WIDE),
        shape(K, PAD),
        shape(K, PAD),
        shape(K, PAD),
        shape(4 * K, PAD),
        shape(K, PAD),
    )
    state = (vectors,)
    made_fields, made_rows, made_images, tables, sigmas, hessen = [], [], [], [], [], []
    for turn in range(STEPS):
        out_shape = (
            shape(count, 1, ORDERS * WIDE),
            shape(2, total, cols),
            shape(16, cells, dtype=BF16),
            shape(rows, cols),
        ) + state_shapes
        if turn:
            out_shape += (shape(8, WIDE), shape(8, PAD), shape(8, PAD))
        else:
            out_shape += (shape(PAD, WIDE),)
        outs = pl.pallas_call(
            functools.partial(turn_body, turn, inverse_total, count),
            out_shape=out_shape,
            scratch_shapes=[
                pltpu.VMEM((5, 2, total, cols), F32),
                pltpu.VMEM((8, total, cols), F32),
                pltpu.VMEM((8, cells), F32),
            ],
            name=f"turn{turn}", compiler_params=LARGE,
        )(parts, *state, tall, side, coefs, split, *made_fields, *made_rows)
        made_fields.append(outs[1])
        made_rows.append(outs[2])
        made_images.append(outs[3])
        state = outs[4:10]
        if turn:
            tables.append(outs[10])
            sigmas.append(outs[11])
            hessen.append(outs[12])
        else:
            folded = outs[10]
        parts = exchange(outs[0])

    new_columns, coefficients, hessenberg, gram, new_images = pl.pallas_call(
        functools.partial(final_body, inverse_total),
        out_shape=(
            shape(STEPS, rows, cols),
            shape(WIDTH, 4, K),
            shape(STEPS, WIDTH),
            shape(ORDERS, ORDERS, K, K),
            shape(STEPS, rows, cols),
        ),
        name="final", compiler_params=SMALL,
    )(parts, *state, folded, *tables, *sigmas, *hessen, *made_fields, *made_images)
    gram = jnp.transpose(gram, (0, 2, 1, 3))
    coefficients = jnp.transpose(coefficients, (1, 2, 0))
    return (new_columns, coefficients, hessenberg, gram, new_images)


def solution(mesh):
    in_specs = (P(None, "row", "col"), P(), P("row", "col"), P("row", "col"))
    out_specs = (P(None, "row", "col"), P(), P(), P(), P(None, "row", "col"))
    return jax.shard_map(local, mesh=mesh, in_specs=in_specs, out_specs=out_specs, check_vma=False)
```

```python
import functools
import jax
import jax.numpy as jnp
from jax import lax
from jax.experimental import pallas as pl
from jax.experimental.pallas import tpu as pltpu
from jax.sharding import PartitionSpec as P

K = 40
STEPS = 3
R = 37
KRYLOV = 34
WIDTH = KRYLOV + STEPS

COUPLING = 0.2
EPSILON = 1e-06
GRAM_SHIFT = 0.05
HIGHEST = lax.Precision.HIGHEST
F32 = jnp.float32
BF16 = jnp.bfloat16

ORDERS = 5
HALO = (ORDERS - 1) * (STEPS + 1)
STRIDE = 48
WIDE = 256
SMALL = pltpu.CompilerParams(vmem_limit_bytes=8 << 20)
LARGE = pltpu.CompilerParams(vmem_limit_bytes=24 << 20)
PAD = 128
AXES = ("row", "col")
NT = (((1,), (1,)), ((), ()))


def device_count():
    return lax.axis_size("row") * lax.axis_size("col")


def exchange(spread):
    return lax.all_to_all(spread, AXES, 0, 0, tiled=True)


def shifts(axis):
    peers = lax.axis_size(axis)
    up = [(i, i + 1) for i in range(peers - 1)]
    return up, [(j, i) for i, j in up]


def lanes(shape):
    return lax.broadcasted_iota(jnp.int32, shape, len(shape) - 1)


def sublanes(shape):
    return lax.broadcasted_iota(jnp.int32, shape, len(shape) - 2)


def pack_body(before_ref, fields_ref, after_ref, low_ref, high_ref):
    rows, slots, cols = fields_ref.shape
    span = cols // HALO
    lane = lanes((slots, cols))
    edge = HALO // span

    def group(source, shift, g, carry):
        low = jnp.zeros((slots, cols), F32)
        high = jnp.zeros((slots, cols), F32)
        for k in range(span):
            cells = source[(g - shift) * span + k]
            inside = (lane >= k * HALO) & (lane < (k + 1) * HALO)
            first = pltpu.roll(cells, k * HALO, 1) if k else cells
            turn = (k * HALO + HALO) % cols
            second = pltpu.roll(cells, turn, 1) if turn else cells
            low = jnp.where(inside, first, low)
            high = jnp.where(inside, second, high)
        low_ref[g] = low
        high_ref[g] = high
        return carry

    last = edge + rows // span
    for g in range(0, edge):
        group(before_ref, 0, g, 0)
    for g in range(edge, last):
        group(fields_ref, edge, g, 0)
    for g in range(last, last + edge):
        group(after_ref, last, g, 0)


def lower_inverse(matrix, count):
    half = PAD // 2
    block = 4
    tile = (8, PAD)
    groups = range(K // 8)
    lane = lanes(tile)
    row = [sublanes(tile) + 8 * g for g in groups]
    work = []
    for g in groups:
        used = (row[g] < count) & (lane < count)
        left = jnp.where(used, matrix[8 * g : 8 * g + 8], (lane == row[g]).astype(F32))
        work.append(jnp.where(lane < half, left, (lane == row[g] + half).astype(F32)))
    for start in range(0, K, block):
        active = [g for g in groups if 8 * g + 7 > start]
        spots = range(start, start + block)
        pivots = [jnp.broadcast_to(work[j // 8][j % 8 : j % 8 + 1], tile) for j in spots]
        below = [
            {g: jnp.broadcast_to(work[g][:, j : j + 1], tile) for g in active} for j in spots
        ]
        corner = [
            [jnp.broadcast_to(pivots[i][:, j : j + 1], tile) for j in spots] for i in range(block)
        ]
        for i in range(block):
            inverse = 1.0 / corner[i][i]
            for k in range(i + 1, block):
                ratio = corner[i][k] * inverse
                pivots[k] = pivots[k] - pivots[i] * ratio
                for g in active:
                    below[k][g] = below[k][g] - below[i][g] * ratio
                for other in range(k, block):
                    corner[k][other] = corner[k][other] - corner[i][other] * ratio
            below[i] = {g: below[i][g] * inverse for g in active}
        for g in active:
            for i in range(block):
                work[g] = work[g] - jnp.where(row[g] > start + i, below[i][g] * pivots[i], 0.0)
    out = []
    for g in groups:
        size = jnp.sum(jnp.where(lane == row[g], work[g], 0.0), axis=1, keepdims=True)
        valid = (row[g] < count) & (lane >= half) & (lane < half + count)
        out.append(pltpu.roll(jnp.where(valid, work[g] / jnp.sqrt(size), 0.0), half, 1))
    return jnp.concatenate(out, 0)


def krylov_body(raw_ref, out_ref):
    groups, length, width = raw_ref.shape
    out_ref[...] = jnp.zeros(out_ref.shape, F32)
    for j in range(groups):
        out_ref[j * K : j * K + length, :width] = raw_ref[j]
    flat = out_ref[...]
    square = lax.dot_general(
        flat, flat, (((0,), (0,)), ((), ())), precision=HIGHEST, preferred_element_type=F32
    )
    inverse = lower_inverse(square[:K], width)
    inverse = jnp.concatenate([inverse, jnp.zeros((PAD - K, PAD), F32)], 0)
    out_ref[...] = lax.dot_general(flat, inverse, NT, precision=HIGHEST, preferred_element_type=F32)


def sideways(main, side, lane):
    cols = main.shape[-1]
    main_up = pltpu.roll(main, 1, 1)
    side_up = pltpu.roll(side, 1, 1)
    main_down = pltpu.roll(main, cols - 1, 1)
    side_down = pltpu.roll(side, cols - 1, 1)
    first = lane == 0
    last = lane == cols - 1
    left = (jnp.where(first, side_up, main_up), jnp.where(first, main_up, side_up))
    right = (jnp.where(last, side_down, main_down), jnp.where(last, main_down, side_down))
    return left, right


def image_body(
    before_ref, fields_ref, after_ref, left_ref, right_ref,
    tall_ref, side_ref, coef_ref, split_ref, gram_ref,
    local_ref, m1, s1, m2, s2, m3, s3, acc_ref,
):
    total, slots, cols = tall_ref.shape
    rows = total - 2 * HALO
    span = cols // HALO
    lane = lanes((slots, cols))

    def unpack(source, shift, g, carry):
        gathered = [[] for _ in range(8)]
        from_left = left_ref[g]
        from_right = right_ref[g]
        for k in range(span):
            r = g * span + k
            main = source[(g - shift) * span + k]
            tall_ref[r] = main
            turn = (cols - k * HALO) % cols
            low = pltpu.roll(from_right, turn, 1) if turn else from_right
            turn = (cols - HALO - k * HALO) % cols
            high = pltpu.roll(from_left, turn, 1) if turn else from_left
            side = jnp.where(lane < HALO, low, jnp.where(lane >= cols - HALO, high, 0.0))
            packed = []
            for cells in (main, side):
                spin = cells[R + 1 : R + 2]
                couple = COUPLING * cells[R + 2 : R + 3]
                packed += [cells[R : R + 1], spin - couple, -spin - couple, couple]
            local_ref[r] = 2.0 * jnp.concatenate(packed, 0)
            for q in range(8):
                gathered[q].append(packed[q])
            side_ref[r] = side
        for q in range(8):
            coef_ref[q, pl.ds(g * span, span), :] = jnp.concatenate(gathered[q], 0)
        return carry

    first = HALO // span
    last = first + rows // span
    for g in range(0, first):
        unpack(before_ref, 0, g, 0)
    for g in range(first, last):
        unpack(fields_ref, first, g, 0)
    for g in range(last, last + first):
        unpack(after_ref, last, g, 0)

    blank = jnp.zeros((STRIDE - slots, cols), F32)
    size = ORDERS * STRIDE

    def keep(order, r, cells):
        whole = jnp.concatenate([cells, blank], 0)
        high = whole.astype(BF16)
        low = (whole - high.astype(F32)).astype(BF16)
        place = slice((r - HALO) * cols, (r - HALO + 1) * cols)
        split_ref[order * STRIDE : (order + 1) * STRIDE, place] = high
        split_ref[size + order * STRIDE : size + (order + 1) * STRIDE, place] = low

    def level(order, source, older, target, need_side):
        source_main, source_side = source

        def one(r, store):
            main = source_main[r]
            side = source_side[r]
            local = local_ref[r]
            left, right = sideways(main, side, lane)
            fresh = (
                local[0:1] * main
                + local[1:2] * right[0]
                + local[2:3] * left[0]
                - local[3:4] * (source_main[r - 1] + source_main[r + 1])
            )
            if order == 1:
                fresh = 0.5 * fresh
            if older is not None:
                fresh = fresh - older[0][r]
            if target is not None:
                target[0][r] = fresh
            if need_side:
                edge = (
                    local[4:5] * side
                    + local[5:6] * right[1]
                    + local[6:7] * left[1]
                    - local[7:8] * (source_side[r - 1] + source_side[r + 1])
                )
                if order == 1:
                    edge = 0.5 * edge
                if older is not None:
                    edge = edge - older[1][r]
                target[1][r] = edge
            if store:
                keep(order, r, fresh)

        reach = ORDERS - 1 - order

        for k in range(reach):
            one(HALO - 1 - k, False)
            one(HALO + rows + k, False)
        for r in range(HALO, HALO + rows):
            one(r, True)

    for r in range(HALO, HALO + rows):
        keep(0, r, tall_ref[r])
    level(1, (tall_ref, side_ref), None, (m1, s1), True)
    level(2, (m1, s1), (tall_ref, side_ref), (m2, s2), True)
    level(3, (m2, s2), (m1, s1), (m3, s3), True)
    level(4, (m3, s3), (m2, s2), None, False)

    acc_ref[:, size:] = jnp.zeros((2 * size, WIDE - size), F32)
    chunk = rows * cols // 3
    for i in range(3):
        place = slice(i * chunk, (i + 1) * chunk)
        part = lax.dot_general(
            split_ref[:, place], split_ref[:size, place], NT, preferred_element_type=F32
        )
        if i:
            acc_ref[:, :size] += part
        else:
            acc_ref[:, :size] = part
    cross = jnp.concatenate(
        [acc_ref[size:, :size], jnp.zeros((size, WIDE - size), F32)], 1
    )
    cross = jnp.concatenate([cross, jnp.zeros((WIDE - size, WIDE), F32)], 0)
    acc_ref[:size, :size] += (cross + jnp.transpose(cross))[:size, :size]
    lane_wide = lanes((K, WIDE))

    def band(order):
        return acc_ref[order * STRIDE : order * STRIDE + K, :]

    bands = [
        band(0),
        jnp.where(lane_wide < STRIDE, pltpu.roll(band(4), WIDE - 4 * STRIDE, 1), band(1)),
        jnp.where(lane_wide < 2 * STRIDE, pltpu.roll(band(3), WIDE - 3 * STRIDE, 1), band(2)),
    ]
    for i in range(3):
        acc_ref[i * K : (i + 1) * K, :] = bands[i]
    count, _, piece = gram_ref.shape
    width = min(piece, WIDE)
    for i in range(count):
        for k in range(0, piece, width):
            spot, start = divmod(i * piece + k, WIDE)
            gram_ref[i, :, k : k + width] = acc_ref[spot : spot + 1, start : start + width]


def relay_body(parts_ref, spread_ref):
    total = jnp.sum(parts_ref[...], axis=0)
    for i in range(spread_ref.shape[0]):
        spread_ref[i] = total


def absorb(parts, state, turn, inverse_total):
    gram, factor, flipped, square, vectors, pending = state
    new_row = R + turn
    column = KRYLOV + turn
    total = jnp.sum(parts, axis=0) * inverse_total
    table = jnp.concatenate(
        [total[:, a * WIDE : (a + 1) * WIDE] for a in range(ORDERS)]
        + [jnp.zeros((8 - ORDERS, WIDE), F32)],
        0,
    )
    lane_one = lanes((1, WIDE))
    norm = jnp.sum(jnp.where(lane_one == new_row, table[0:1], 0.0), axis=1, keepdims=True)
    beta = jnp.sqrt(norm + EPSILON)
    sigma = 1.0 / beta
    here = (lanes((K, PAD)) == new_row) & (sublanes((K, PAD)) == new_row)
    factor = jnp.where(here, sigma, factor)
    flipped = jnp.where(here, sigma, flipped)
    square = jnp.where(here, sigma * sigma, square)
    tall = jnp.transpose(
        jnp.concatenate([table[:, :PAD], jnp.zeros((PAD - 8, PAD), F32)], 0)
    )
    lane_gram = lanes((K, WIDE))
    gram = jnp.where(sublanes((K, WIDE)) == new_row, table[0:1], gram)
    for b in range(ORDERS):
        gram = jnp.where(lane_gram == b * STRIDE + new_row, tall[:K, b : b + 1], gram)

    latest = [vectors[j * K : (j + 1) * K, column - 1 : column] for j in range(4)]
    unit = (lax.broadcasted_iota(jnp.int32, (K, 1), 0) == new_row).astype(F32)
    expanded = jnp.concatenate(
        [
            latest[1],
            0.5 * (latest[0] + latest[2]),
            0.5 * (latest[1] + latest[3]),
            pending + beta * unit,
        ],
        0,
    )
    first = jnp.sum(vectors * expanded, axis=0, keepdims=True)
    ortho = expanded - jnp.sum(vectors * first, axis=1, keepdims=True)
    second = jnp.sum(vectors * ortho, axis=0, keepdims=True)
    ortho = ortho - jnp.sum(vectors * second, axis=1, keepdims=True)
    eta = jnp.sqrt(jnp.sum(ortho * ortho, axis=0, keepdims=True) + EPSILON)
    vectors = jnp.where(lanes((4 * K, PAD)) == column, ortho / eta, vectors)
    hessenberg = first + second + eta * (lanes((1, PAD)) == column).astype(F32)
    return (gram, factor, flipped, square, vectors, pending), table, sigma, hessenberg


def coefficients_of(state, turn):
    gram, factor, flipped, square, vectors, _ = state
    column = KRYLOV + turn
    latest = [vectors[j * K : (j + 1) * K, column - 1 : column] for j in range(4)]
    mixes = [jnp.sum(factor * one, axis=0, keepdims=True) for one in latest]
    wide = [jnp.concatenate([m, jnp.zeros((1, WIDE - PAD), F32)], 1) for m in mixes]
    target = 0.5 * wide[2]
    for j in range(4):
        target = target - pltpu.roll(0.5 * wide[j], (j + 1) * STRIDE, 1)
    raw = jnp.sum(gram * target, axis=1, keepdims=True)
    upper = jnp.sum(square * raw, axis=0, keepdims=True)
    inside = jnp.where(lanes((K, PAD)) < K, gram[:, :PAD], 0.0)
    twice = 2.0 * raw - jnp.sum(inside * upper, axis=1, keepdims=True)
    removed = jnp.sum(square * twice, axis=0, keepdims=True)
    pending = jnp.sum(
        jnp.where(lanes((K, PAD)) == sublanes((K, PAD)), jnp.sum(flipped * twice, axis=0, keepdims=True), 0.0),
        axis=1,
        keepdims=True,
    )
    table = jnp.concatenate(mixes + [removed] + [jnp.zeros((PAD - 5, PAD), F32)], 0)
    return jnp.transpose(table), mixes + [removed], pending


def turn_body(turn, inverse_total, count, *refs):
    refs = list(refs)
    parts_ref = refs.pop(0)
    state_refs = [refs.pop(0) for _ in range(6 if turn else 1)]
    main_ref, side_ref, coef_ref, split_ref = [refs.pop(0) for _ in range(4)]
    old_fields = [refs.pop(0) for _ in range(turn)]
    old_rows = [refs.pop(0) for _ in range(turn)]
    spread_ref, field_ref, rows_ref, image_ref = [refs.pop(0) for _ in range(4)]
    out_state = [refs.pop(0) for _ in range(6)]
    if turn:
        table_ref, sigma_ref, hessenberg_ref = [refs.pop(0) for _ in range(3)]
    else:
        folded_ref = refs.pop(0)
    z_ref, t_ref, flat_ref = refs

    if turn:
        state = tuple(r[...] for r in state_refs[:5]) + (state_refs[5][:, 0:1],)
        state, table, sigma, hessenberg = absorb(parts_ref[...], state, turn - 1, inverse_total)
        table_ref[...] = table
        sigma_ref[...] = jnp.broadcast_to(sigma, sigma_ref.shape)
        hessenberg_ref[...] = jnp.broadcast_to(hessenberg, hessenberg_ref.shape)
    else:
        pieces, _, piece = parts_ref.shape
        width = min(piece, WIDE)
        for i in range(pieces):
            for k in range(0, piece, width):
                spot, start = divmod(i * piece + k, WIDE)
                folded_ref[spot : spot + 1, start : start + width] = (
                    parts_ref[i, :, k : k + width] * inverse_total
                )
        gram = folded_ref[0:K, :]
        diagonal = lanes((K, PAD)) == sublanes((K, PAD))
        factor = lower_inverse(gram[:, :PAD] + jnp.where(diagonal, GRAM_SHIFT, 0.0), R)
        square = lax.dot_general(
            factor, factor, (((0,), (0,)), ((), ())), precision=HIGHEST, preferred_element_type=F32
        )[:K]
        flipped = jnp.transpose(jnp.concatenate([factor, jnp.zeros((PAD - K, PAD), F32)], 0))[:K]
        state = (gram, factor, flipped, square, state_refs[0][...], None)
    upright, mixes, pending = coefficients_of(state, turn)
    for ref, value in zip(out_state[:5], state[:5]):
        ref[...] = value
    out_state[5][...] = jnp.broadcast_to(pending, out_state[5].shape)

    total, slots, cols = main_ref.shape
    rows = total - 2 * HALO
    raw_only = sublanes((K, cols)) < R
    weights = [jnp.where(raw_only, upright[:K, j : j + 1], 0.0) for j in range(5)]

    def mix_group(g):
        for half, ref in enumerate((main_ref, side_ref)):
            lists = [[] for _ in range(5)]
            for k in range(8):
                cells = ref[g * 8 + k]
                for j in range(5):
                    lists[j].append(jnp.sum(weights[j] * cells, axis=0, keepdims=True))
            for j in range(5):
                z_ref[j, half, pl.ds(pl.multiple_of(g * 8, 8), 8), :] = jnp.concatenate(lists[j], 0)

    def mix(i, carry):
        for k in range(groups):
            mix_group(idle + i * groups + k)
        return carry

    idle = (ORDERS - 1) * turn // 8
    groups = (total // 8 - 2 * idle) // 2
    if idle:
        z_ref[:, :, : 8 * idle] = jnp.zeros((5, 2, 8 * idle, cols), F32)
        z_ref[:, :, total - 8 * idle :] = jnp.zeros((5, 2, 8 * idle, cols), F32)
    lax.fori_loop(0, 2, mix, 0)

    z = []
    for j in range(5):
        pair = [z_ref[j, 0], z_ref[j, 1]]
        for s in range(turn):
            scale = mixes[j][:, R + s : R + s + 1]
            pair = [pair[half] + scale * old_fields[s][half] for half in range(2)]
        z.append(pair)

    lane = lanes((total, cols))
    local = [coef_ref[q] for q in range(8)]

    def operate(pair):
        main, side = pair
        left, right = sideways(main, side, lane)
        out = []
        for half, cells in enumerate(pair):
            c = local[4 * half : 4 * half + 4]
            out.append(
                c[0] * cells
                + c[1] * right[half]
                + c[2] * left[half]
                - c[3] * (pltpu.roll(cells, 1, 0) + pltpu.roll(cells, total - 1, 0))
            )
        return out

    def combine(*terms):
        return [sum(w * p[half] for w, p in terms) for half in range(2)]

    four = z[3]
    three = combine((1.0, z[2]), (2.0, operate(four)))
    two = combine((1.0, z[1]), (2.0, operate(three)), (-1.0, four))
    one = combine((1.0, z[0]), (2.0, operate(two)), (-1.0, three))
    summed = combine((1.0, operate(one)), (-1.0, two))
    field = combine((0.5, z[2]), (-0.5, summed), (-1.0, z[4]))
    field_ref[0] = field[0]
    field_ref[1] = field[1]

    images = [field, operate(field)]
    for _ in range(ORDERS - 2):
        images.append(combine((2.0, operate(images[-1])), (-1.0, images[-2])))
    for a in range(ORDERS):
        t_ref[a] = images[a][0]
    image_ref[...] = t_ref[ORDERS - 1, HALO : HALO + rows, :]
    t_ref[ORDERS:] = jnp.zeros((8 - ORDERS, total, cols), F32)
    for r in range(rows):
        flat_ref[:, r * cols : (r + 1) * cols] = t_ref[:, HALO + r, :]

    size = ORDERS * STRIDE
    chunk = rows * cols // 3
    table = jnp.zeros((2 * size, 16), F32)
    own = jnp.zeros((16, 16 * (turn + 1)), F32)
    for i in range(3):
        place = slice(i * chunk, (i + 1) * chunk)
        mine = flat_ref[:, place]
        rounded = mine.astype(BF16).astype(F32)
        both = jnp.concatenate([rounded, mine - rounded], 0).astype(BF16)
        rows_ref[:, place] = both
        table = table + lax.dot_general(
            split_ref[:, place], both, NT, preferred_element_type=F32
        )
        others = jnp.concatenate([ref[:, place] for ref in old_rows] + [both], 0)
        own = own + lax.dot_general(both, others, NT, preferred_element_type=F32)
    own = [
        own[0:8, 16 * s : 16 * s + 8]
        + own[0:8, 16 * s + 8 : 16 * s + 16]
        + own[8:16, 16 * s : 16 * s + 8]
        for s in range(turn + 1)
    ]
    table = table[:size, 0:8] + table[:size, 8:16] + table[size:, 0:8]
    table = jnp.concatenate([table, jnp.zeros((size, PAD - 8), F32)], 1)
    table = jnp.transpose(jnp.concatenate([table, jnp.zeros((WIDE - size, PAD), F32)], 0))[:8]
    lane_table = lanes((8, WIDE))
    for s in range(turn + 1):
        for b in range(ORDERS):
            table = jnp.where(
                lane_table == b * STRIDE + R + s, own[s][:, b : b + 1], table
            )
    flat = jnp.concatenate([table[a : a + 1] for a in range(ORDERS)], 1)
    for i in range(count):
        spread_ref[i] = flat


def final_body(inverse_total, *refs):
    refs = list(refs)
    parts_ref = refs.pop(0)
    state_refs = [refs.pop(0) for _ in range(6)]
    folded_ref = refs.pop(0)
    old_tables = [refs.pop(0) for _ in range(STEPS - 1)]
    old_sigmas = [refs.pop(0) for _ in range(STEPS - 1)]
    old_hessen = [refs.pop(0) for _ in range(STEPS - 1)]
    fields = [refs.pop(0) for _ in range(STEPS)]
    images = [refs.pop(0) for _ in range(STEPS)]
    columns_ref, coefficients_ref, hessenberg_ref, gram_ref, image_ref = refs

    state = tuple(r[...] for r in state_refs[:5]) + (state_refs[5][:, 0:1],)
    state, table, sigma, hessenberg = absorb(parts_ref[...], state, STEPS - 1, inverse_total)
    factor = state[1]
    flat = jnp.concatenate([state[4], jnp.zeros((WIDE - 4 * K, PAD), F32)], 0)
    flat = jnp.transpose(flat)[:WIDTH]
    for j in range(4):
        coefficients_ref[:, j, :] = flat[:, j * K : (j + 1) * K]
    hessenberg_ref[...] = jnp.concatenate([r[0:1] for r in old_hessen] + [hessenberg], 0)[:, :WIDTH]
    sigmas = [ref[0:1, 0:1] for ref in old_sigmas] + [sigma]
    rows = columns_ref.shape[1]
    for s in range(STEPS):
        columns_ref[s] = sigmas[s] * fields[s][0, HALO : HALO + rows, :]
        image_ref[s] = sigmas[s] * images[s][...]

    lane_wide = lanes((K, WIDE))
    bands = [folded_ref[i * K : (i + 1) * K, :] for i in range(3)]
    upper = [
        bands[0],
        bands[1],
        bands[2],
        pltpu.roll(bands[2], 3 * STRIDE, 1),
        pltpu.roll(bands[1], 4 * STRIDE, 1),
    ]
    blank = jnp.zeros((STRIDE - K, WIDE), F32)
    stacked = []
    for a in range(ORDERS):
        stacked += [jnp.where((lane_wide >= a * STRIDE) & (lane_wide < ORDERS * STRIDE), upper[a], 0.0), blank]
    whole = jnp.concatenate(stacked + [jnp.zeros((WIDE - ORDERS * STRIDE, WIDE), F32)], 0)
    row_id = sublanes((WIDE, WIDE))
    lane_id = lanes((WIDE, WIDE))
    lower = row_id >= (lane_id // STRIDE + 1) * STRIDE
    whole = jnp.where(lower, jnp.transpose(whole), whole)
    for s, one in enumerate([ref[...] for ref in old_tables] + [table]):
        flipped = jnp.transpose(jnp.concatenate([one, jnp.zeros((PAD - 8, WIDE), F32)], 0))
        for a in range(ORDERS):
            whole = jnp.where(row_id == a * STRIDE + R + s, one[a : a + 1, :], whole)
        for a in range(ORDERS):
            whole = jnp.where(lane_id == a * STRIDE + R + s, flipped[:, a : a + 1], whole)
    padded = jnp.concatenate([factor, jnp.zeros((K, WIDE - PAD), F32)], 1)
    padded = jnp.concatenate([padded, blank], 0)
    blocks = [padded] + [pltpu.roll(padded, a * STRIDE, 1) for a in range(1, ORDERS)]
    diagonal = jnp.concatenate(blocks + [jnp.zeros((WIDE - ORDERS * STRIDE, WIDE), F32)], 0)
    half = jnp.dot(diagonal, whole, precision=HIGHEST, preferred_element_type=F32)
    done = lax.dot_general(half, diagonal, NT, precision=HIGHEST, preferred_element_type=F32)
    for a in range(ORDERS):
        for b in range(ORDERS):
            gram_ref[a, b] = done[a * STRIDE : a * STRIDE + K, b * STRIDE : b * STRIDE + K]


def shape(*dims, dtype=F32):
    return jax.ShapeDtypeStruct(dims, dtype)


def local(basis_raw, krylov_raw, stiffness, rotation):
    rows = basis_raw.shape[1]
    cols = basis_raw.shape[2]
    cells = rows * cols
    count = device_count()
    inverse_total = 1.0 / (cells * count)
    total = rows + 2 * HALO
    size = ORDERS * STRIDE

    fields = jnp.concatenate(
        [
            jnp.transpose(basis_raw, (1, 0, 2)),
            stiffness[:, None],
            rotation[:, None],
            jnp.ones((rows, 1, cols), F32),
        ],
        1,
    )
    up, down = shifts("row")
    before = lax.ppermute(fields[rows - HALO :], "row", up)
    after = lax.ppermute(fields[:HALO], "row", down)
    pieces = (before, fields, after)
    strip = shape(total * HALO // cols, K, cols)
    low, high = pl.pallas_call(pack_body, out_shape=(strip, strip), name="pack", compiler_params=SMALL)(*pieces)
    up, down = shifts("col")
    from_left = lax.ppermute(high, "col", up)
    from_right = lax.ppermute(low, "col", down)
    vectors = pl.pallas_call(krylov_body, out_shape=shape(4 * K, PAD), name="krylov", compiler_params=SMALL)(krylov_raw)
    vectors, from_left = lax.optimization_barrier((vectors, from_left))

    level = pltpu.VMEM((total, K, cols), F32)
    piece = PAD * WIDE // count
    tall, side, coefs, split, folded = pl.pallas_call(
        image_body,
        out_shape=(
            shape(total, K, cols),
            shape(total, K, cols),
            shape(8, total, cols),
            shape(2 * size, cells, dtype=BF16),
            shape(count, 1, piece),
        ),
        scratch_shapes=[pltpu.VMEM((total, 8, cols), F32)]
        + [level] * 6
        + [pltpu.VMEM((2 * size, WIDE), F32)],
        name="images", compiler_params=LARGE,
    )(*pieces, from_left, from_right)

    mine = pl.pallas_call(
        relay_body, out_shape=shape(count, 1, piece), name="relay", compiler_params=SMALL
    )(exchange(folded))
    parts = exchange(mine)

    state_shapes = (
        shape(K, WIDE),
        shape(K, PAD),
        shape(K, PAD),
        shape(K, PAD),
        shape(4 * K, PAD),
        shape(K, PAD),
    )
    state = (vectors,)
    made_fields, made_rows, made_images, tables, sigmas, hessen = [], [], [], [], [], []
    for turn in range(STEPS):
        out_shape = (
            shape(count, 1, ORDERS * WIDE),
            shape(2, total, cols),
            shape(16, cells, dtype=BF16),
            shape(rows, cols),
        ) + state_shapes
        if turn:
            out_shape += (shape(8, WIDE), shape(8, PAD), shape(8, PAD))
        else:
            out_shape += (shape(PAD, WIDE),)
        outs = pl.pallas_call(
            functools.partial(turn_body, turn, inverse_total, count),
            out_shape=out_shape,
            scratch_shapes=[
                pltpu.VMEM((5, 2, total, cols), F32),
                pltpu.VMEM((8, total, cols), F32),
                pltpu.VMEM((8, cells), F32),
            ],
            name=f"turn{turn}", compiler_params=LARGE,
        )(parts, *state, tall, side, coefs, split, *made_fields, *made_rows)
        made_fields.append(outs[1])
        made_rows.append(outs[2])
        made_images.append(outs[3])
        state = outs[4:10]
        if turn:
            tables.append(outs[10])
            sigmas.append(outs[11])
            hessen.append(outs[12])
        else:
            folded = outs[10]
        parts = exchange(outs[0])

    new_columns, coefficients, hessenberg, gram, new_images = pl.pallas_call(
        functools.partial(final_body, inverse_total),
        out_shape=(
            shape(STEPS, rows, cols),
            shape(WIDTH, 4, K),
            shape(STEPS, WIDTH),
            shape(ORDERS, ORDERS, K, K),
            shape(STEPS, rows, cols),
        ),
        name="final", compiler_params=SMALL,
    )(parts, *state, folded, *tables, *sigmas, *hessen, *made_fields, *made_images)
    gram = jnp.transpose(gram, (0, 2, 1, 3))
    coefficients = jnp.transpose(coefficients, (1, 2, 0))
    return (new_columns, coefficients, hessenberg, gram, new_images)


def solution(mesh):
    in_specs = (P(None, "row", "col"), P(), P("row", "col"), P("row", "col"))
    out_specs = (P(None, "row", "col"), P(), P(), P(), P(None, "row", "col"))
    return jax.shard_map(local, mesh=mesh, in_specs=in_specs, out_specs=out_specs, check_vma=False)
```
